8 devices in a mesh: dp: 1 (over z), tp: 8 (over y, x, core).
Axes of the slice: x: 2, y: 2, z: 1, core: 2. Of those that a mesh axis runs over, the one named last changes fastest.
Arguments:
- hidden: bfloat16 [128, 2048], P('dp')
- w_gate: bfloat16 [2048, 8192], P(None, 'tp')
- w_up: bfloat16 [2048, 8192], P(None, 'tp')
- w_down: bfloat16 [8192, 2048], P('tp')
- norm_gain: float32 [2048], replicated
- w_vocab: bfloat16 [2048, 49152], P(None, 'tp')
- temperature: float32 [128], P('dp')
- target: int32 [128], P('dp')
Outputs:
- output 1: float32 [128], P('dp')
- output 2: float32 [128], P('dp')
- output 3: float32 [128], P('dp')
- output 4: bfloat16 [128, 49152], P('dp')
All inputs are finite; a program needn't handle non-finite values.
Results may differ from the reference program's by a relative error of at most 0.00406014.
Values are sent between devices in bfloat16 or wider.
A program may use at most 1 GiB of HBM per device.

```python
import jax
import jax.numpy as jnp
from jax import lax

MODEL_DIM = 2048
FF_DIM = 8192
VOCAB_SIZE = 49152
BATCH_ROWS = 128
ROW_BLOCK = min(32, BATCH_ROWS)
NORM_EPS = 1e-6


def setup_inputs(seed: int = 0, part: int = 0) -> dict:
    shared_keys = jax.random.split(jax.random.key(seed), 5)
    part_keys = jax.random.split(jax.random.fold_in(jax.random.key(seed + 1), part), 3)
    hidden = jax.random.normal(part_keys[0], (BATCH_ROWS, MODEL_DIM), jnp.float32)
    w_gate = jax.random.normal(shared_keys[0], (MODEL_DIM, FF_DIM), jnp.float32) * MODEL_DIM ** -0.5
    w_up = jax.random.normal(shared_keys[1], (MODEL_DIM, FF_DIM), jnp.float32) * MODEL_DIM ** -0.5
    w_down = jax.random.normal(shared_keys[2], (FF_DIM, MODEL_DIM), jnp.float32) * (2.0 * FF_DIM ** -0.5)
    norm_gain = jax.random.uniform(shared_keys[3], (MODEL_DIM,), jnp.float32, 0.5, 1.5)
    w_vocab = jax.random.normal(shared_keys[4], (MODEL_DIM, VOCAB_SIZE), jnp.float32) * (1.5 * MODEL_DIM ** -0.5)
    temperature = jax.random.uniform(part_keys[1], (BATCH_ROWS,), jnp.float32, 0.5, 2.0)
    target = jax.random.randint(part_keys[2], (BATCH_ROWS,), 0, VOCAB_SIZE, jnp.int32)
    return {
        "hidden": hidden.astype(jnp.bfloat16),
        "w_gate": w_gate.astype(jnp.bfloat16),
        "w_up": w_up.astype(jnp.bfloat16),
        "w_down": w_down.astype(jnp.bfloat16),
        "norm_gain": norm_gain,
        "w_vocab": w_vocab.astype(jnp.bfloat16),
        "temperature": temperature,
        "target": target,
    }


def reference(hidden, w_gate, w_up, w_down, norm_gain, w_vocab, temperature, target):
    block_count = hidden.shape[0] // ROW_BLOCK
    hidden_blocks = hidden.reshape(block_count, ROW_BLOCK, hidden.shape[1])
    temp_blocks = temperature.reshape(block_count, ROW_BLOCK)
    target_blocks = target.reshape(block_count, ROW_BLOCK)
    vocab_ids = jnp.arange(w_vocab.shape[1], dtype=jnp.int32)

    def one_block(block):
        hidden_rows, temp_rows, target_rows = block
        gate_pre = jnp.dot(hidden_rows, w_gate, preferred_element_type=jnp.float32)
        up_pre = jnp.dot(hidden_rows, w_up, preferred_element_type=jnp.float32)
        hidden_act = (jax.nn.silu(gate_pre) * up_pre).astype(jnp.bfloat16)
        mlp_out = jnp.dot(hidden_act, w_down, preferred_element_type=jnp.float32)
        residual = hidden_rows.astype(jnp.float32) + mlp_out
        inv_rms = lax.rsqrt(jnp.mean(residual * residual, axis=-1, keepdims=True) + NORM_EPS)
        normed = (norm_gain * residual * inv_rms).astype(jnp.bfloat16)
        logits = jnp.dot(normed, w_vocab, preferred_element_type=jnp.float32) / temp_rows[:, None]
        row_max = jnp.max(logits, axis=-1, keepdims=True)
        shifted = jnp.exp(logits - row_max)
        sum_exp = jnp.sum(shifted, axis=-1)
        log_norm = row_max[:, 0] + jnp.log(sum_exp)
        entropy = log_norm - jnp.sum(shifted * logits, axis=-1) / sum_exp
        target_logit = jnp.sum(jnp.where(vocab_ids[None, :] == target_rows[:, None], logits, 0.0), axis=-1)
        log_probs = (logits - log_norm[:, None]).astype(jnp.bfloat16)
        return log_norm, entropy, target_logit - log_norm, log_probs

    log_norm, entropy, target_logp, log_probs = lax.map(one_block, (hidden_blocks, temp_blocks, target_blocks))
    return (
        log_norm.reshape(-1),
        entropy.reshape(-1),
        target_logp.reshape(-1),
        log_probs.reshape(-1, w_vocab.shape[1]),
    )
```

```python
import jax
import jax.numpy as jnp
from jax import lax
from jax.experimental import pallas as pl
from jax.experimental.pallas import tpu as pltpu
from jax.sharding import PartitionSpec as P

NORM_EPS = 1e-6
F32 = jnp.float32
BF16 = jnp.bfloat16
B, D, FL, V, VL = 128, 2048, 1024, 49152, 6144
NC = 12
CW = VL // NC
EARLY = 3
NF = 4
FW = FL // NF
NJ = 2
JW = D // NJ
HALF, PIECE = 64, 16


def _lanes(row):
    return jnp.transpose(jnp.broadcast_to(row, (128, 128)))


def _main(hid_hbm, wg_hbm, wu_hbm, wd_hbm, gain_ref, wv_hbm, temp_ref, tgt_ref,
          out, small,
          w, wv, hid, act, yf, ysend, yrecv, psend, precv, xbuf, statm, stats, offs, invt, tgtm,
          in_sem, wf_sem, wd_sem, wv_sem,
          d2d_s, d2d_r, rs_s, rs_r, xa_s, xa_r, xf_s, xf_r, st_s, st_r,
          own_s, fwd_s, par_s, rx, ry, rd, pr):
    me = lax.axis_index("tp")
    core, chip = me % 2, me // 2
    nx, ny, nd, pt = me ^ 2, me ^ 4, me ^ 6, me ^ 1

    def remote(src, dst, ss, rs, dev):
        return pltpu.make_async_remote_copy(src, dst, ss, rs, device_id={"tp": dev})

    hid_copy = pltpu.make_async_copy(hid_hbm, hid, in_sem)
    hid_copy.start()
    wf_copies = []
    for b in range(NF):
        for t, ref in enumerate((wg_hbm, wu_hbm)):
            c = pltpu.make_async_copy(ref.at[:, pl.ds(b * FW, FW)], w.at[:, pl.ds(t * FL + b * FW, FW)], wf_sem.at[t, b])
            c.start()
            wf_copies.append(c)
    wd_copies = []
    for j in range(NJ):
        c = pltpu.make_async_copy(wd_hbm.at[:, pl.ds(j * JW, JW)], w.at[pl.ds(j * FL, FL), pl.ds(2 * FL, JW)], wd_sem.at[j])
        c.start()
        wd_copies.append(c)

    barrier = pltpu.get_barrier_semaphore()
    for k in range(1, 8):
        pl.semaphore_signal(barrier, inc=1, device_id={"tp": me ^ k})

    invt[...] = _lanes(1.0 / temp_ref[...])
    tgtm[...] = _lanes(tgt_ref[...].astype(F32)).astype(jnp.int32)

    hid_copy.wait()
    for b in range(NF):
        wf_copies[2 * b].wait()
        wf_copies[2 * b + 1].wait()
        g = jnp.dot(hid[...], w[:, b * FW:(b + 1) * FW], preferred_element_type=F32)
        u = jnp.dot(hid[...], w[:, FL + b * FW:FL + (b + 1) * FW], preferred_element_type=F32)
        act[:, b * FW:(b + 1) * FW] = (jax.nn.silu(g) * u).astype(BF16)

    keep = pl.multiple_of(core * HALF, HALF)
    give = pl.multiple_of(HALF - core * HALF, HALF)
    d2d = []
    for j in range(NJ):
        cols = pl.ds(j * JW, JW)
        wd_copies[j].wait()
        yf[:, j * JW:(j + 1) * JW] = jnp.dot(act[...], w[j * FL:(j + 1) * FL, 2 * FL:2 * FL + JW], preferred_element_type=F32)
        ysend[:, j * JW:(j + 1) * JW] = yf[pl.ds(give, HALF), j * JW:(j + 1) * JW].astype(BF16)
        if j == 0:
            pl.semaphore_wait(barrier, 7)
        c = remote(ysend.at[:, cols], yrecv.at[:, cols], d2d_s.at[j], d2d_r.at[j], pt)
        c.start()
        d2d.append(c)

    wv_copies = []
    for i in range(NC):
        c = pltpu.make_async_copy(wv_hbm.at[:, pl.ds(i * CW, CW)], wv.at[:, pl.ds(i * CW, CW)], wv_sem.at[i])
        c.start()
        wv_copies.append(c)

    def piece(dev):
        return pl.multiple_of((dev // 2) * PIECE, PIECE)

    rs = []
    for j in range(NJ):
        cols = slice(j * JW, (j + 1) * JW)
        d2d[j].wait_recv()
        part = yf[pl.ds(keep, HALF), cols] + yrecv[:, cols].astype(F32)
        yf[pl.ds(keep, HALF), cols] = part
        psend[:, cols] = part.astype(BF16)
        for s, dev in enumerate((nd, nx, ny)):
            c = remote(psend.at[pl.ds(piece(dev), PIECE), pl.ds(j * JW, JW)], precv.at[s, :, pl.ds(j * JW, JW)],
                       rs_s.at[s, j], rs_r.at[s, j], dev)
            c.start()
            rs.append(c)

    def rows_of(dev):
        return pl.multiple_of((dev % 2) * HALF + (dev // 2) * PIECE, PIECE)

    mine = rows_of(me)
    for c in rs:
        c.wait_recv()
    y = yf[pl.ds(mine, PIECE), :]
    for s in range(3):
        y = y + precv[s].astype(F32)
    res = hid[pl.ds(mine, PIECE), :].astype(F32) + y
    inv_rms = lax.rsqrt(jnp.mean(res * res, axis=-1, keepdims=True) + NORM_EPS)
    xbuf[pl.ds(mine, PIECE), :] = (gain_ref[...] * res * inv_rms).astype(BF16)

    def xrow(dev):
        return xbuf.at[pl.ds(rows_of(dev), PIECE), :]

    xs = []
    for s, dev in enumerate((nd, nx, ny)):
        xs.append(remote(xrow(me), xrow(me), xa_s.at[s], xa_r.at[s], dev))
    xs.append(remote(xrow(me), xrow(me), xf_s.at[3], xf_r.at[3], pt))
    for c in xs:
        c.start()
    xf = []
    for s, dev in ((1, nx), (2, ny), (0, nd)):
        remote(xrow(dev), xrow(dev), xa_s.at[s], xa_r.at[s], dev).wait_recv()
        c = remote(xrow(dev), xrow(dev), xf_s.at[s], xf_r.at[s], pt)
        c.start()
        xf.append(c)
    for s, dev in ((3, pt), (1, pt ^ 2), (2, pt ^ 4), (0, pt ^ 6)):
        remote(xrow(dev), xrow(dev), xf_s.at[s], xf_r.at[s], pt).wait_recv()

    def chunk(dev, i):
        row = pl.multiple_of((dev * 2 + i // 6) * 128, 128)
        col = pl.multiple_of((i % 6) * CW, CW)
        return w.at[pl.ds(row, 128), pl.ds(col, CW)]

    def own_copies(i):
        return (remote(chunk(me, i), chunk(me, i), own_s.at[0, i], rx.at[i], nx),
                remote(chunk(me, i), chunk(me, i), own_s.at[1, i], ry.at[i], ny),
                remote(chunk(me, i), chunk(me, i), own_s.at[2, i], pr.at[0, i], pt))

    lane = lax.broadcasted_iota(jnp.int32, (128, 128), 1)
    statm[...] = jnp.zeros((128, 128), F32)

    def head(i, _):
        pltpu.make_async_copy(wv_hbm.at[:, pl.ds(pl.multiple_of(i * CW, CW), CW)],
                              wv.at[:, pl.ds(pl.multiple_of(i * CW, CW), CW)], wv_sem.at[i]).wait()
        acc = jnp.dot(xbuf[...], wv[:, pl.ds(pl.multiple_of(i * CW, CW), CW)], preferred_element_type=F32)
        parts = [acc[:, q * 128:(q + 1) * 128] * invt[...] for q in range(CW // 128)]
        top = parts[0]
        for p in parts[1:]:
            top = jnp.maximum(top, p)
        top = jnp.max(top, axis=-1, keepdims=True)
        ref = chunk(me, i)
        for q, p in enumerate(parts):
            ref[:, q * 128:(q + 1) * 128] = (p - top).astype(BF16)

        @pl.when(i < EARLY)
        def _():
            for c in own_copies(i):
                c.start()

        total = weighted = hit = jnp.zeros((128, 128), F32)
        ids = tgtm[...] - (me * VL + i * CW)
        for q, p in enumerate(parts):
            e = jnp.exp(p - top)
            total = total + e
            weighted = weighted + e * p
            hit = hit + jnp.where(ids == lane + q * 128, p, 0.0)
        sm = statm[...]
        sm = jnp.where(lane == i, top, sm)
        sm = jnp.where(lane == 16 + i, jnp.sum(total, axis=-1, keepdims=True), sm)
        sm = jnp.where(lane == 32 + i, jnp.sum(weighted, axis=-1, keepdims=True), sm)
        sm = jnp.where(lane == 48 + i, jnp.sum(hit, axis=-1, keepdims=True), sm)
        statm[...] = sm
        return 0

    lax.fori_loop(0, NC, head, 0)

    st = jnp.transpose(statm[...])
    tops = st[0:NC, :]
    top = jnp.max(tops, axis=0, keepdims=True)
    scale = jnp.exp(tops - top)
    my_stats = jnp.concatenate(
        [tops, top, jnp.sum(scale * st[16:16 + NC, :], axis=0, keepdims=True),
         jnp.sum(scale * st[32:32 + NC, :], axis=0, keepdims=True),
         jnp.sum(st[48:48 + NC, :], axis=0, keepdims=True)], axis=0)

    def slot(dev):
        return stats.at[pl.ds(pl.multiple_of(dev * 16, 16), 16), :]

    slot(me)[...] = my_stats
    sts = []
    for k in range(1, 8):
        c = remote(slot(me), slot(me), st_s.at[k], st_r.at[k], me ^ k)
        c.start()
        sts.append(c)

    def send_rest(i, _):
        for c in own_copies(i):
            c.start()
        return 0

    lax.fori_loop(EARLY, NC, send_rest, 0)

    for k in range(1, 8):
        remote(slot(me ^ k), slot(me ^ k), st_s.at[k], st_r.at[k], me ^ k).wait_recv()
    allst = [stats[16 * k:16 * (k + 1), :] for k in range(8)]
    top = allst[0][12:13, :]
    for s in allst[1:]:
        top = jnp.maximum(top, s[12:13, :])
    total = weighted = hit = jnp.zeros((1, 128), F32)
    for s in allst:
        scale = jnp.exp(s[12:13, :] - top)
        total = total + scale * s[13:14, :]
        weighted = weighted + scale * s[14:15, :]
        hit = hit + s[15:16, :]
    log_norm = top + jnp.log(total)
    small[0:1, :] = log_norm
    small[1:2, :] = log_norm - weighted / total
    small[2:3, :] = hit - log_norm
    small[3:8, :] = jnp.zeros((5, 128), F32)
    offs[...] = jnp.transpose(stats[...] - log_norm)

    def fix(dev, i):
        off = jnp.sum(jnp.where(lane == dev * 16 + i, offs[...], 0.0), axis=-1, keepdims=True)
        val = chunk(dev, i)[...].astype(F32) + off
        out[:, pl.ds(pl.multiple_of(dev * VL + i * CW, CW), CW)] = val.astype(BF16)

    def from_partner(j, dev, i):
        remote(chunk(dev, i), chunk(dev, i), par_s.at[0, i], pr.at[j, i], pt).wait_recv()
        fix(dev, i)

    def to_partner(j, dev, i):
        remote(chunk(dev, i), chunk(dev, i), par_s.at[j, i], pr.at[j + 1, i], pt).start()

    def relay(dev, i, to):
        return remote(chunk(dev, i), chunk(dev, i), fwd_s.at[i], rd.at[i], to)

    def arrivals(i, _):
        remote(chunk(nx, i), chunk(nx, i), own_s.at[0, i], rx.at[i], nx).wait_recv()

        @pl.when(i % 2 == 0)
        def _():
            relay(nx, i, ny).start()

        to_partner(0, nx, i)
        remote(chunk(ny, i), chunk(ny, i), own_s.at[1, i], ry.at[i], ny).wait_recv()

        @pl.when(i % 2 == 1)
        def _():
            relay(ny, i, nx).start()

        to_partner(1, ny, i)
        fix(me, i)
        fix(nx, i)
        fix(ny, i)
        from_partner(0, pt, i)
        from_partner(1, pt ^ 2, i)
        from_partner(2, pt ^ 4, i)
        return 0

    lax.fori_loop(0, NC, arrivals, 0)

    def diagonal(i, _):
        remote(chunk(nd, i), chunk(nd, i), fwd_s.at[i], rd.at[i], nx).wait_recv()
        to_partner(2, nd, i)
        fix(nd, i)
        from_partner(3, pt ^ 6, i)
        return 0

    lax.fori_loop(0, NC, diagonal, 0)

    def drain(i, _):
        for c in own_copies(i):
            c.wait_send()
        relay(nx, i, ny).wait_send()
        for j, dev in enumerate((nx, ny, nd)):
            remote(chunk(dev, i), chunk(dev, i), par_s.at[j, i], pr.at[j + 1, i], pt).wait_send()
        return 0

    lax.fori_loop(0, NC, drain, 0)
    for c in d2d + rs + xs + xf + sts:
        c.wait_send()


def _write(src, small, out, o0, o1, o2, sem):
    step = B // 8
    cs = [pltpu.make_async_copy(src.at[pl.ds(k * step, step)], out.at[pl.ds(k * step, step)], sem.at[k]) for k in range(8)]
    for c in cs:
        c.start()
    o0[...] = small[0:1, :]
    o1[...] = small[1:2, :]
    o2[...] = small[2:3, :]
    for c in cs:
        c.wait()


def solution(mesh):
    vmem = pl.BlockSpec(memory_space=pltpu.VMEM)
    hbm = pl.BlockSpec(memory_space=pltpu.HBM)
    dma = pltpu.SemaphoreType.DMA

    def device_step(hidden, w_gate, w_up, w_down, norm_gain, w_vocab, temperature, target):
        wide, small = pl.pallas_call(
            _main,
            out_shape=(pltpu.VMEM((B, V), BF16), pltpu.VMEM((8, 128), F32)),
            in_specs=[hbm, hbm, hbm, hbm, vmem, hbm, vmem, vmem],
            out_specs=(vmem, vmem),
            scratch_shapes=[
                pltpu.VMEM((2048, 3072), BF16), pltpu.VMEM((D, VL), BF16), pltpu.VMEM((B, D), BF16),
                pltpu.VMEM((B, FL), BF16), pltpu.VMEM((B, D), F32), pltpu.VMEM((HALF, D), BF16),
                pltpu.VMEM((HALF, D), BF16), pltpu.VMEM((HALF, D), BF16), pltpu.VMEM((3, PIECE, D), BF16),
                pltpu.VMEM((B, D), BF16), pltpu.VMEM((128, 128), F32), pltpu.VMEM((128, 128), F32),
                pltpu.VMEM((128, 128), F32), pltpu.VMEM((128, 128), F32), pltpu.VMEM((128, 128), jnp.int32),
                dma, dma((2, NF)), dma((NJ,)), dma((NC,)),
                dma((NJ,)), dma((NJ,)), dma((3, NJ)), dma((3, NJ)), dma((3,)), dma((3,)), dma((4,)), dma((4,)),
                dma((8,)), dma((8,)),
                dma((3, NC)), dma((NC,)), dma((3, NC)), dma((NC,)), dma((NC,)), dma((NC,)), dma((4, NC)),
            ],
            compiler_params=pltpu.CompilerParams(collective_id=0, has_side_effects=True, vmem_limit_bytes=49 << 20),
            name="step",
        )(hidden, w_gate, w_up, w_down, norm_gain.reshape(1, D), w_vocab, temperature.reshape(1, B), target.reshape(1, B))
        row = jax.ShapeDtypeStruct((1, B), F32)
        log_probs, log_norm, entropy, target_logp = pl.pallas_call(
            _write,
            out_shape=(jax.ShapeDtypeStruct((B, V), BF16), row, row, row),
            in_specs=[vmem, vmem],
            out_specs=(hbm, vmem, vmem, vmem),
            scratch_shapes=[dma((8,))],
            compiler_params=pltpu.CompilerParams(vmem_limit_bytes=16 << 20),
            name="write",
        )(wide, small)
        return log_norm.reshape(B), entropy.reshape(B), target_logp.reshape(B), log_probs

    return jax.shard_map(
        device_step,
        mesh=mesh,
        in_specs=(P("dp", None), P(None, "tp"), P(None, "tp"), P("tp", None), P(None),
                  P(None, "tp"), P("dp"), P("dp")),
        out_specs=(P("dp"), P("dp"), P("dp"), P("dp", None)),
        check_vma=False,
    )
```

```python
import jax
import jax.numpy as jnp
from jax import lax
from jax.experimental import pallas as pl
from jax.experimental.pallas import tpu as pltpu
from jax.sharding import PartitionSpec as P

NORM_EPS = 1e-6
F32 = jnp.float32
BF16 = jnp.bfloat16
B, D, FL, V, VL = 128, 2048, 1024, 49152, 6144
NC = 8
CW = VL // NC
GRID = 3072 // CW
EARLY = 3
NF = 4
FW = FL // NF
NJ = 2
JW = D // NJ
HALF, PIECE = 64, 16
NW = 4
WW = VL // NW


def _lanes(row):
    return jnp.transpose(jnp.broadcast_to(row, (128, 128)))


def _main(hid_hbm, wg_hbm, wu_hbm, wd_hbm, gain_hbm, wv_hbm, temp_hbm, tgt_hbm,
          out, small,
          w, wv, hid, act, yf, ysend, yrecv, psend, precv, xbuf, statm, stats, offs, invt, tgtm, gain, temp, tgt,
          in_sem, wf_sem, wd_sem, wv_sem,
          d2d_s, d2d_r, rs_s, rs_r, x_s, xa_r, xf_r, st_s, st_r, bulk_s, rxy, rd, pr, prd):
    me = lax.axis_index("tp")
    core = me % 2
    nx, ny, nd, pt = me ^ 2, me ^ 4, me ^ 6, me ^ 1

    def remote(src, dst, ss, rs, dev):
        return pltpu.make_async_remote_copy(src, dst, ss, rs, device_id={"tp": dev})

    def load(src, dst, sem):
        c = pltpu.make_async_copy(src, dst, sem)
        c.start()
        return c

    def load_wf(b):
        for t, ref in enumerate((wg_hbm, wu_hbm)):
            load(ref.at[:, pl.ds(b * FW, FW)], w.at[:, pl.ds(t * FL + b * FW, FW)], wf_sem.at[b])

    def wait_wf(b):
        both = w.at[:, pl.ds(0, 2 * FW)]
        pltpu.make_async_copy(wv_hbm.at[:, pl.ds(0, 2 * FW)], both, wf_sem.at[b]).wait()

    def load_wd(j):
        return load(wd_hbm.at[:, pl.ds(j * JW, JW)], w.at[pl.ds(j * FL, FL), pl.ds(2 * FL, JW)], wd_sem.at[j])

    def load_wv(n):
        return load(wv_hbm.at[:, pl.ds(n * WW, WW)], wv.at[:, pl.ds(n * WW, WW)], wv_sem.at[n])

    hid_copy = load(hid_hbm, hid, in_sem.at[0])
    load_wf(0)
    small_copies = [load(temp_hbm, temp, in_sem.at[1]), load(tgt_hbm, tgt, in_sem.at[2]), load(gain_hbm, gain, in_sem.at[3])]
    load_wf(1)

    barrier = pltpu.get_barrier_semaphore()
    for k in range(1, 8):
        pl.semaphore_signal(barrier, inc=1, device_id={"tp": me ^ k})

    hid_copy.wait()
    wd_copies, wv_copies = [], []
    for b in range(NF):
        wait_wf(b)
        if b < NF - 2:
            load_wf(b + 2)
        else:
            wd_copies.append(load_wd(b - NF + 2))
        g = jnp.dot(hid[...], w[:, b * FW:(b + 1) * FW], preferred_element_type=F32)
        u = jnp.dot(hid[...], w[:, FL + b * FW:FL + (b + 1) * FW], preferred_element_type=F32)
        act[:, b * FW:(b + 1) * FW] = (jax.nn.silu(g) * u).astype(BF16)

    keep = pl.multiple_of(core * HALF, HALF)
    give = pl.multiple_of(HALF - core * HALF, HALF)
    d2d = []
    for j in range(NJ):
        cols = pl.ds(j * JW, JW)
        wd_copies[j].wait()
        wv_copies.append(load_wv(j))
        yf[:, j * JW:(j + 1) * JW] = jnp.dot(act[...], w[j * FL:(j + 1) * FL, 2 * FL:2 * FL + JW], preferred_element_type=F32)
        ysend[:, j * JW:(j + 1) * JW] = yf[pl.ds(give, HALF), j * JW:(j + 1) * JW].astype(BF16)
        if j == 0:
            pl.semaphore_wait(barrier, 7)
        c = remote(ysend.at[:, cols], yrecv.at[:, cols], d2d_s, d2d_r.at[j], pt)
        c.start()
        d2d.append(c)

    def rows_of(dev):
        return pl.multiple_of((dev % 2) * HALF + (dev // 2) * PIECE, PIECE)

    for c in small_copies:
        c.wait()
    offs[...] = _lanes(1.0 / temp[...])
    statm[...] = _lanes(tgt[...].astype(F32))
    for k in range(8):
        rows = pl.ds(rows_of(me ^ k), PIECE)
        invt[k * PIECE:(k + 1) * PIECE, :] = offs[rows, :]
        tgtm[k * PIECE:(k + 1) * PIECE, :] = statm[rows, :].astype(jnp.int32)

    def piece(dev):
        return pl.multiple_of((dev // 2) * PIECE, PIECE)

    for j in range(NJ):
        cols = slice(j * JW, (j + 1) * JW)
        d2d[j].wait_recv()
        part = yf[pl.ds(keep, HALF), cols] + yrecv[:, cols].astype(F32)
        yf[pl.ds(keep, HALF), cols] = part
        psend[:, cols] = part.astype(BF16)
        for s, dev in enumerate((nd, nx, ny)):
            remote(psend.at[pl.ds(piece(dev), PIECE), pl.ds(j * JW, JW)], precv.at[pl.ds(s * PIECE, PIECE), pl.ds(j * JW, JW)],
                   rs_s, rs_r, dev).start()
    for n in range(NJ, NW):
        wv_copies.append(load_wv(n))

    rs_all = remote(precv, precv, rs_s, rs_r, nx)
    rs_all.wait_recv()
    mine = rows_of(me)
    y = yf[pl.ds(mine, PIECE), :]
    for s in range(3):
        y = y + precv[s * PIECE:(s + 1) * PIECE, :].astype(F32)
    res = hid[pl.ds(mine, PIECE), :].astype(F32) + y
    inv_rms = lax.rsqrt(jnp.mean(res * res, axis=-1, keepdims=True) + NORM_EPS)
    xbuf[0:PIECE, :] = (gain[...] * res * inv_rms).astype(BF16)

    def xrow(k):
        return xbuf.at[pl.ds(k * PIECE, PIECE), :]

    for s, k in enumerate((6, 2, 4)):
        remote(xrow(0), xrow(k), x_s, xa_r.at[s], me ^ k).start()
    remote(xrow(0), xrow(1), x_s, xf_r, pt).start()

    def place(dev, i):
        row = pl.multiple_of((dev * 2 + i // GRID) * 128, 128)
        col = pl.multiple_of((i % GRID) * CW, CW)
        return row, pl.ds(col, CW)

    def chunk(dev, i):
        row, cols = place(dev, i)
        return w.at[pl.ds(row, 128), cols]

    def own_start(i, first, count):
        row, cols = place(me, i)
        ref = w.at[pl.ds(row + first, count), cols]
        remote(ref, ref, bulk_s, rxy.at[i], nx).start()
        remote(ref, ref, bulk_s, rxy.at[i], ny).start()
        remote(ref, ref, bulk_s, pr.at[i], pt).start()

    def head(i, first, count):
        acc = jnp.dot(xbuf[first:first + count, :], wv[:, pl.ds(pl.multiple_of(i * CW, CW), CW)], preferred_element_type=F32)
        scale = invt[first:first + count, :]
        parts = [acc[:, q * 128:(q + 1) * 128] * scale for q in range(CW // 128)]
        top = parts[0]
        for p in parts[1:]:
            top = jnp.maximum(top, p)
        top = jnp.max(top, axis=-1, keepdims=True)
        row, _ = place(me, i)
        for q, p in enumerate(parts):
            w[pl.ds(row + first, count), pl.ds(pl.multiple_of((i % GRID) * CW + q * 128, 128), 128)] = (p - top).astype(BF16)
        if first == 0:
            own_start(i, first, count)
        else:
            @pl.when(i < EARLY)
            def _():
                own_start(i, first, count)

        total = weighted = hit = jnp.zeros((count, 128), F32)
        lane = lax.broadcasted_iota(jnp.int32, (count, 128), 1)
        ids = tgtm[first:first + count, :] - (me * VL + i * CW)
        for q, p in enumerate(parts):
            e = jnp.exp(p - top)
            total = total + e
            weighted = weighted + e * p
            hit = hit + jnp.where(ids == lane + q * 128, p, 0.0)
        sm = statm[first:first + count, :]
        sm = jnp.where(lane == i, top, sm)
        sm = jnp.where(lane == 16 + i, jnp.sum(total, axis=-1, keepdims=True), sm)
        sm = jnp.where(lane == 32 + i, jnp.sum(weighted, axis=-1, keepdims=True), sm)
        sm = jnp.where(lane == 48 + i, jnp.sum(hit, axis=-1, keepdims=True), sm)
        statm[first:first + count, :] = sm

    def head_own(i, _):
        head(i, 0, PIECE)
        return 0

    def head_rest(i, _):
        head(i, PIECE, B - PIECE)
        return 0

    for c in wv_copies:
        c.wait()
    lax.fori_loop(0, NC, head_own, 0)
    for s, k in ((1, 2), (2, 4), (0, 6)):
        remote(xrow(k), xrow(k), x_s, xa_r.at[s], me ^ k).wait_recv()
        remote(xrow(k), xrow(k + 1), x_s, xf_r, pt).start()
    four = xbuf.at[pl.ds(0, 4 * PIECE), :]
    remote(four, four, x_s, xf_r, pt).wait_recv()
    lax.fori_loop(0, NC, head_rest, 0)

    for k in range(8):
        offs[pl.ds(rows_of(me ^ k), PIECE), :] = statm[k * PIECE:(k + 1) * PIECE, :]
    st = jnp.transpose(offs[...])
    tops = st[0:NC, :]
    top = jnp.max(tops, axis=0, keepdims=True)
    scale = jnp.exp(tops - top)
    my_stats = jnp.concatenate(
        [tops, top, jnp.sum(scale * st[16:16 + NC, :], axis=0, keepdims=True),
         jnp.sum(scale * st[32:32 + NC, :], axis=0, keepdims=True),
         jnp.sum(st[48:48 + NC, :], axis=0, keepdims=True),
         jnp.zeros((16 - NC - 4, 128), F32)], axis=0)

    stats[0:16, :] = my_stats
    for k in range(1, 8):
        remote(stats.at[pl.ds(0, 16), :], stats.at[pl.ds(16 * k, 16), :], st_s, st_r, me ^ k).start()

    def send_rest(i, _):
        own_start(i, PIECE, B - PIECE)
        return 0

    lax.fori_loop(EARLY, NC, send_rest, 0)

    others = stats.at[pl.ds(16, 112), :]
    st_all = remote(others, others, st_s, st_r, nx)
    st_all.wait_recv()
    allst = [stats[16 * k:16 * (k + 1), :] for k in range(8)]
    top = allst[0][NC:NC + 1, :]
    for s in allst[1:]:
        top = jnp.maximum(top, s[NC:NC + 1, :])
    total = weighted = hit = jnp.zeros((1, 128), F32)
    for s in allst:
        scale = jnp.exp(s[NC:NC + 1, :] - top)
        total = total + scale * s[NC + 1:NC + 2, :]
        weighted = weighted + scale * s[NC + 2:NC + 3, :]
        hit = hit + s[NC + 3:NC + 4, :]
    log_norm = top + jnp.log(total)
    small[0:1, :] = log_norm
    small[1:2, :] = log_norm - weighted / total
    small[2:3, :] = hit - log_norm
    small[3:8, :] = jnp.zeros((5, 128), F32)
    offs[...] = jnp.transpose(stats[...] - log_norm)

    lane16 = lax.broadcasted_iota(jnp.int32, (PIECE, 128), 1)

    def fix(rel, i):
        dev = me ^ rel
        row, cols = place(dev, i)
        for k in range(8):
            rows = pl.ds(rows_of(dev ^ k), PIECE)
            off = jnp.sum(jnp.where(lane16 == rel * 16 + i, offs[rows, :], 0.0), axis=-1, keepdims=True)
            val = w[pl.ds(row + k * PIECE, PIECE), cols].astype(F32) + off
            out[rows, pl.ds(pl.multiple_of(dev * VL + i * CW, CW), CW)] = val.astype(BF16)

    def land(n):
        return w.at[pl.ds(0, n * 128), pl.ds(0, CW)]

    def arrived(n, sem):
        remote(land(n), land(n), bulk_s, sem, nx).wait_recv()

    def forward(rel, i, sem, to):
        ref = chunk(me ^ rel, i)
        remote(ref, ref, bulk_s, sem, to).start()

    def arrivals(i, _):
        arrived(2, rxy.at[i])

        @pl.when(i % 2 == 0)
        def _():
            forward(2, i, rd.at[i], ny)

        @pl.when(i % 2 == 1)
        def _():
            forward(4, i, rd.at[i], nx)

        forward(2, i, pr.at[i], pt)
        forward(4, i, pr.at[i], pt)
        fix(0, i)
        fix(2, i)
        fix(4, i)
        arrived(3, pr.at[i])
        fix(1, i)
        fix(3, i)
        fix(5, i)
        return 0

    lax.fori_loop(0, NC, arrivals, 0)

    def diagonal(i, _):
        arrived(1, rd.at[i])
        forward(6, i, prd.at[i], pt)
        fix(6, i)
        arrived(1, prd.at[i])
        fix(7, i)
        return 0

    lax.fori_loop(0, NC, diagonal, 0)

    def left(ref, sem):
        remote(ref, ref, sem, rs_r, nx).wait_send()

    left(ysend, d2d_s)
    rs_all.wait_send()
    left(xbuf.at[pl.ds(0, 7 * PIECE), :], x_s)
    st_all.wait_send()
    left(w.at[pl.ds(0, 1792), :], bulk_s)


def _write(src, small, out, o0, o1, o2, sem):
    step = B // 8
    cs = [pltpu.make_async_copy(small.at[pl.ds(k, 1), :], o, sem.at[8 + k]) for k, o in enumerate((o0, o1, o2))]
    cs += [pltpu.make_async_copy(src.at[pl.ds(k * step, step)], out.at[pl.ds(k * step, step)], sem.at[k]) for k in range(8)]
    for c in cs:
        c.start()
    for c in cs:
        c.wait()


def solution(mesh):
    vmem = pl.BlockSpec(memory_space=pltpu.VMEM)
    hbm = pl.BlockSpec(memory_space=pltpu.HBM)
    dma = pltpu.SemaphoreType.DMA

    def device_step(hidden, w_gate, w_up, w_down, norm_gain, w_vocab, temperature, target):
        wide, small = pl.pallas_call(
            _main,
            out_shape=(pltpu.VMEM((B, V), BF16), pltpu.VMEM((8, 128), F32)),
            in_specs=[hbm] * 8,
            out_specs=(vmem, vmem),
            scratch_shapes=[
                pltpu.VMEM((2048, 3072), BF16), pltpu.VMEM((D, VL), BF16), pltpu.VMEM((B, D), BF16),
                pltpu.VMEM((B, FL), BF16), pltpu.VMEM((B, D), F32), pltpu.VMEM((HALF, D), BF16),
                pltpu.VMEM((HALF, D), BF16), pltpu.VMEM((HALF, D), BF16), pltpu.VMEM((3 * PIECE, D), BF16),
                pltpu.VMEM((B, D), BF16), pltpu.VMEM((128, 128), F32), pltpu.VMEM((128, 128), F32),
                pltpu.VMEM((128, 128), F32), pltpu.VMEM((128, 128), F32), pltpu.VMEM((128, 128), jnp.int32),
                pltpu.VMEM((1, D), F32), pltpu.VMEM((1, B), F32), pltpu.VMEM((1, B), jnp.int32),
                dma((4,)), dma((NF,)), dma((NJ,)), dma((NW,)),
                dma, dma((NJ,)), dma, dma, dma, dma((3,)), dma, dma, dma, dma,
                dma((NC,)), dma((NC,)), dma((NC,)), dma((NC,)),
            ],
            compiler_params=pltpu.CompilerParams(collective_id=0, has_side_effects=True, vmem_limit_bytes=49 << 20),
            name="step",
        )(hidden, w_gate, w_up, w_down, norm_gain.reshape(1, D), w_vocab, temperature.reshape(1, B), target.reshape(1, B))
        row = jax.ShapeDtypeStruct((1, B), F32)
        log_probs, log_norm, entropy, target_logp = pl.pallas_call(
            _write,
            out_shape=(jax.ShapeDtypeStruct((B, V), BF16), row, row, row),
            in_specs=[vmem, vmem],
            out_specs=(hbm, hbm, hbm, hbm),
            scratch_shapes=[dma((11,))],
            compiler_params=pltpu.CompilerParams(vmem_limit_bytes=16 << 20),
            name="write",
        )(wide, small)
        return log_norm.reshape(B), entropy.reshape(B), target_logp.reshape(B), log_probs

    return jax.shard_map(
        device_step,
        mesh=mesh,
        in_specs=(P("dp", None), P(None, "tp"), P(None, "tp"), P("tp", None), P(None),
                  P(None, "tp"), P("dp"), P("dp")),
        out_specs=(P("dp"), P("dp"), P("dp"), P("dp", None)),
        check_vma=False,
    )
```

```python
import jax
import jax.numpy as jnp
from jax import lax
from jax.experimental import pallas as pl
from jax.experimental.pallas import tpu as pltpu
from jax.sharding import PartitionSpec as P

NORM_EPS = 1e-6
F32 = jnp.float32
BF16 = jnp.bfloat16
B, D, FL, V, VL = 128, 2048, 1024, 49152, 6144
NC = 8
CW = VL // NC
GRID = 3072 // CW
EARLY = 3
OWN = 5
SPLIT = 6
NS = 2
NF = 4
FW = FL // NF
NJ = 2
JW = D // NJ
HALF, PIECE = 64, 16
NW = 4
WW = VL // NW


def _lanes(row):
    return jnp.transpose(jnp.broadcast_to(row, (128, 128)))


def _main(hid_hbm, wg_hbm, wu_hbm, wd_hbm, gain_hbm, wv_hbm, temp_hbm, tgt_hbm,
          out, small,
          w, wv, hid, act, yf, ysend, yrecv, psend, precv, xbuf, statm, stats, offs, invt, tgtm, gain, temp, tgt,
          in_sem, wf_sem, wd_sem, wv_sem,
          d2d_s, d2d_r, rs_s, rs_r, x_s, xa_r, xf_r, st_s, st_r, bulk_s, rxy, rd, pr, prd):
    me = lax.axis_index("tp")
    core = me % 2
    nx, ny, nd, pt = me ^ 2, me ^ 4, me ^ 6, me ^ 1

    def remote(src, dst, ss, rs, dev):
        return pltpu.make_async_remote_copy(src, dst, ss, rs, device_id={"tp": dev})

    def load(src, dst, sem):
        c = pltpu.make_async_copy(src, dst, sem)
        c.start()
        return c

    def load_wf(b):
        for t, ref in enumerate((wg_hbm, wu_hbm)):
            load(ref.at[:, pl.ds(b * FW, FW)], w.at[:, pl.ds(t * FL + b * FW, FW)], wf_sem.at[b])

    def wait_wf(b):
        both = w.at[:, pl.ds(0, 2 * FW)]
        pltpu.make_async_copy(wv_hbm.at[:, pl.ds(0, 2 * FW)], both, wf_sem.at[b]).wait()

    def load_wd(j):
        return load(wd_hbm.at[:, pl.ds(j * JW, JW)], w.at[pl.ds(j * FL, FL), pl.ds(2 * FL, JW)], wd_sem.at[j])

    def load_wv(n):
        return load(wv_hbm.at[:, pl.ds(n * WW, WW)], wv.at[:, pl.ds(n * WW, WW)], wv_sem.at[n])

    hid_copy = load(hid_hbm, hid, in_sem.at[0])
    load_wf(0)
    small_copies = [load(temp_hbm, temp, in_sem.at[1]), load(tgt_hbm, tgt, in_sem.at[2]), load(gain_hbm, gain, in_sem.at[3])]
    load_wf(1)

    barrier = pltpu.get_barrier_semaphore()
    for k in range(1, 8):
        pl.semaphore_signal(barrier, inc=1, device_id={"tp": me ^ k})

    hid_copy.wait()
    wd_copies, wv_copies = [], []
    for b in range(NF):
        wait_wf(b)
        if b < NF - 2:
            load_wf(b + 2)
        else:
            wd_copies.append(load_wd(b - NF + 2))
            if b == NF - 1:
                wv_copies.append(load_wv(0))
        g = jnp.dot(hid[...], w[:, b * FW:(b + 1) * FW], preferred_element_type=F32)
        u = jnp.dot(hid[...], w[:, FL + b * FW:FL + (b + 1) * FW], preferred_element_type=F32)
        act[:, b * FW:(b + 1) * FW] = (jax.nn.silu(g) * u).astype(BF16)

    keep = pl.multiple_of(core * HALF, HALF)
    give = pl.multiple_of(HALF - core * HALF, HALF)
    d2d = []
    for j in range(NJ):
        cols = pl.ds(j * JW, JW)
        wd_copies[j].wait()
        wv_copies.append(load_wv(j + 1))
        yf[:, j * JW:(j + 1) * JW] = jnp.dot(act[...], w[j * FL:(j + 1) * FL, 2 * FL:2 * FL + JW], preferred_element_type=F32)
        ysend[:, j * JW:(j + 1) * JW] = yf[pl.ds(give, HALF), j * JW:(j + 1) * JW].astype(BF16)
        if j == 0:
            pl.semaphore_wait(barrier, 7)
        c = remote(ysend.at[:, cols], yrecv.at[:, cols], d2d_s, d2d_r.at[j], pt)
        c.start()
        d2d.append(c)

    def rows_of(dev):
        return pl.multiple_of((dev % 2) * HALF + (dev // 2) * PIECE, PIECE)

    for n in range(NJ + 1, NW):
        wv_copies.append(load_wv(n))
    for c in small_copies:
        c.wait()
    offs[...] = _lanes(1.0 / temp[...])
    statm[...] = _lanes(tgt[...].astype(F32))
    for k in range(8):
        rows = pl.ds(rows_of(me ^ k), PIECE)
        invt[k * PIECE:(k + 1) * PIECE, :] = offs[rows, :]
        tgtm[k * PIECE:(k + 1) * PIECE, :] = statm[rows, :].astype(jnp.int32)

    def piece(dev):
        return pl.multiple_of((dev // 2) * PIECE, PIECE)

    for j in range(NJ):
        cols = slice(j * JW, (j + 1) * JW)
        d2d[j].wait_recv()
        part = yf[pl.ds(keep, HALF), cols] + yrecv[:, cols].astype(F32)
        yf[pl.ds(keep, HALF), cols] = part
        psend[:, cols] = part.astype(BF16)
        for s, dev in enumerate((nd, nx, ny)):
            remote(psend.at[pl.ds(piece(dev), PIECE), pl.ds(j * JW, JW)], precv.at[pl.ds(s * PIECE, PIECE), pl.ds(j * JW, JW)],
                   rs_s, rs_r, dev).start()
    rs_all = remote(precv, precv, rs_s, rs_r, nx)
    rs_all.wait_recv()
    mine = rows_of(me)
    y = yf[pl.ds(mine, PIECE), :]
    for s in range(3):
        y = y + precv[s * PIECE:(s + 1) * PIECE, :].astype(F32)
    res = hid[pl.ds(mine, PIECE), :].astype(F32) + y
    inv_rms = lax.rsqrt(jnp.mean(res * res, axis=-1, keepdims=True) + NORM_EPS)
    xbuf[0:PIECE, :] = (gain[...] * res * inv_rms).astype(BF16)

    def xrow(k):
        return xbuf.at[pl.ds(k * PIECE, PIECE), :]

    for s, k in enumerate((6, 2, 4)):
        remote(xrow(0), xrow(k), x_s, xa_r.at[s], me ^ k).start()
    remote(xrow(0), xrow(1), x_s, xf_r, pt).start()

    def place(dev, i):
        row = pl.multiple_of((dev * 2 + i // GRID) * 128, 128)
        col = pl.multiple_of((i % GRID) * CW, CW)
        return row, pl.ds(col, CW)

    def chunk(dev, i):
        row, cols = place(dev, i)
        return w.at[pl.ds(row, 128), cols]

    def own_start(i, first, count):
        row, cols = place(me, i)
        ref = w.at[pl.ds(row + first, count), cols]
        remote(ref, ref, bulk_s, rxy.at[i], nx).start()
        remote(ref, ref, bulk_s, rxy.at[i], ny).start()
        remote(ref, ref, bulk_s, pr.at[i], pt).start()

    def head(i, first, count):
        acc = jnp.dot(xbuf[first:first + count, :], wv[:, pl.ds(pl.multiple_of(i * CW, CW), CW)], preferred_element_type=F32)
        scale = invt[first:first + count, :]
        parts = [acc[:, q * 128:(q + 1) * 128] * scale for q in range(CW // 128)]
        top = parts[0]
        for p in parts[1:]:
            top = jnp.maximum(top, p)
        top = jnp.max(top, axis=-1, keepdims=True)
        row, _ = place(me, i)
        for q, p in enumerate(parts):
            w[pl.ds(row + first, count), pl.ds(pl.multiple_of((i % GRID) * CW + q * 128, 128), 128)] = (p - top).astype(BF16)
        if count == PIECE:
            own_start(i, first, count)
        elif first:
            @pl.when(i < EARLY)
            def _():
                own_start(i, first, count)

        total = weighted = hit = jnp.zeros((count, 128), F32)
        lane = lax.broadcasted_iota(jnp.int32, (count, 128), 1)
        ids = tgtm[first:first + count, :] - (me * VL + i * CW)
        for q, p in enumerate(parts):
            e = jnp.exp(p - top)
            total = total + e
            weighted = weighted + e * p
            hit = hit + jnp.where(ids == lane + q * 128, p, 0.0)
        sm = statm[first:first + count, :]
        sm = jnp.where(lane == i, top, sm)
        sm = jnp.where(lane == 16 + i, jnp.sum(total, axis=-1, keepdims=True), sm)
        sm = jnp.where(lane == 32 + i, jnp.sum(weighted, axis=-1, keepdims=True), sm)
        sm = jnp.where(lane == 48 + i, jnp.sum(hit, axis=-1, keepdims=True), sm)
        statm[first:first + count, :] = sm

    def head_own(i, _):
        head(i, 0, PIECE)
        return 0

    def head_rest(i, _):
        head(i, PIECE, B - PIECE)
        return 0

    def head_all(i, _):
        head(i, 0, B)
        return 0

    ready = 0
    for i in range(OWN):
        while ready * WW < (i + 1) * CW:
            wv_copies[ready].wait()
            ready += 1
        head_own(i, 0)
    for s, k in ((1, 2), (2, 4), (0, 6)):
        remote(xrow(k), xrow(k), x_s, xa_r.at[s], me ^ k).wait_recv()
        remote(xrow(k), xrow(k + 1), x_s, xf_r, pt).start()
    four = xbuf.at[pl.ds(0, 4 * PIECE), :]
    remote(four, four, x_s, xf_r, pt).wait_recv()
    for c in wv_copies[ready:]:
        c.wait()
    lax.fori_loop(0, OWN, head_rest, 0)
    lax.fori_loop(OWN, NC, head_all, 0)

    for k in range(8):
        offs[pl.ds(rows_of(me ^ k), PIECE), :] = statm[k * PIECE:(k + 1) * PIECE, :]
    st = jnp.transpose(offs[...])
    tops = st[0:NC, :]
    top = jnp.max(tops, axis=0, keepdims=True)
    scale = jnp.exp(tops - top)
    my_stats = jnp.concatenate(
        [tops, top, jnp.sum(scale * st[16:16 + NC, :], axis=0, keepdims=True),
         jnp.sum(scale * st[32:32 + NC, :], axis=0, keepdims=True),
         jnp.sum(st[48:48 + NC, :], axis=0, keepdims=True),
         jnp.zeros((16 - NC - 4, 128), F32)], axis=0)

    stats[0:16, :] = my_stats
    for k in range(1, 8):
        remote(stats.at[pl.ds(0, 16), :], stats.at[pl.ds(16 * k, 16), :], st_s, st_r, me ^ k).start()

    def send_rest(i, _):
        own_start(i, PIECE, B - PIECE)
        return 0

    def send_all(i, _):
        own_start(i, 0, B)
        return 0

    lax.fori_loop(EARLY, OWN, send_rest, 0)
    lax.fori_loop(OWN, NC, send_all, 0)

    others = stats.at[pl.ds(16, 112), :]
    st_all = remote(others, others, st_s, st_r, nx)
    st_all.wait_recv()
    allst = [stats[16 * k:16 * (k + 1), :] for k in range(8)]
    top = allst[0][NC:NC + 1, :]
    for s in allst[1:]:
        top = jnp.maximum(top, s[NC:NC + 1, :])
    total = weighted = hit = jnp.zeros((1, 128), F32)
    for s in allst:
        scale = jnp.exp(s[NC:NC + 1, :] - top)
        total = total + scale * s[NC + 1:NC + 2, :]
        weighted = weighted + scale * s[NC + 2:NC + 3, :]
        hit = hit + s[NC + 3:NC + 4, :]
    log_norm = top + jnp.log(total)
    small[0:1, :] = log_norm
    small[1:2, :] = log_norm - weighted / total
    small[2:3, :] = hit - log_norm
    small[3:8, :] = jnp.zeros((5, 128), F32)
    offs[...] = jnp.transpose(stats[...] - log_norm)

    lane16 = lax.broadcasted_iota(jnp.int32, (PIECE, 128), 1)

    def fix(rel, i, first=0, count=8):
        dev = me ^ rel
        row, cols = place(dev, i)
        for k in range(first, first + count):
            rows = pl.ds(rows_of(dev ^ k), PIECE)
            off = jnp.sum(jnp.where(lane16 == rel * 16 + i, offs[rows, :], 0.0), axis=-1, keepdims=True)
            val = w[pl.ds(row + k * PIECE, PIECE), cols].astype(F32) + off
            out[rows, pl.ds(pl.multiple_of(dev * VL + i * CW, CW), CW)] = val.astype(BF16)

    def land(n):
        return w.at[pl.ds(0, n * 128), pl.ds(0, CW)]

    def arrived(n, sem):
        remote(land(n), land(n), bulk_s, sem, nx).wait_recv()

    def forward(rel, i, sem, to):
        ref = chunk(me ^ rel, i)
        remote(ref, ref, bulk_s, sem, to).start()

    def pieces(rel, i, n):
        row, cols = place(me ^ rel, i)
        return w.at[pl.ds(row + n * (128 // NS), 128 // NS), cols]

    def piece_sem(sems, i, n):
        return sems.at[i if n == 0 else NC + (i - SPLIT) * (NS - 1) + n - 1]

    def relay(rel, i, to):
        if isinstance(i, int):
            for n in range(NS):
                ref = pieces(rel, i, n)
                remote(ref, ref, bulk_s, piece_sem(rd, i, n), to).start()
        else:
            forward(rel, i, rd.at[i], to)

    def arrivals(i, _):
        arrived(2, rxy.at[i])
        if isinstance(i, int):
            relay(2, i, ny) if i % 2 == 0 else relay(4, i, nx)
        else:
            @pl.when(i % 2 == 0)
            def _():
                relay(2, i, ny)

            @pl.when(i % 2 == 1)
            def _():
                relay(4, i, nx)

        forward(2, i, pr.at[i], pt)
        forward(4, i, pr.at[i], pt)
        fix(0, i)
        fix(2, i)
        fix(4, i)
        arrived(3, pr.at[i])
        fix(1, i)
        fix(3, i)
        fix(5, i)
        return 0

    lax.fori_loop(0, SPLIT, arrivals, 0)
    for i in range(SPLIT, NC):
        arrivals(i, 0)

    def diagonal(i, _):
        arrived(1, rd.at[i])
        forward(6, i, prd.at[i], pt)
        fix(6, i)
        arrived(1, prd.at[i])
        fix(7, i)
        return 0

    lax.fori_loop(0, SPLIT, diagonal, 0)
    quarter = w.at[pl.ds(0, 128 // NS), pl.ds(0, CW)]
    for n in range(NS):
        for i in range(SPLIT, NC):
            remote(quarter, quarter, bulk_s, piece_sem(rd, i, n), nx).wait_recv()
            ref = pieces(6, i, n)
            remote(ref, ref, bulk_s, piece_sem(prd, i, n), pt).start()
            fix(6, i, 8 // NS * n, 8 // NS)
    for n in range(NS):
        for i in range(SPLIT, NC):
            remote(quarter, quarter, bulk_s, piece_sem(prd, i, n), pt).wait_recv()
            fix(7, i, 8 // NS * n, 8 // NS)

    def left(ref, sem):
        remote(ref, ref, sem, rs_r, nx).wait_send()

    left(ysend, d2d_s)
    rs_all.wait_send()
    left(xbuf.at[pl.ds(0, 7 * PIECE), :], x_s)
    st_all.wait_send()
    left(w.at[pl.ds(0, 1792), :], bulk_s)


def _write(src, small, out, o0, o1, o2, sem):
    step = B // 8
    cs = [pltpu.make_async_copy(small.at[pl.ds(k, 1), :], o, sem.at[8 + k]) for k, o in enumerate((o0, o1, o2))]
    cs += [pltpu.make_async_copy(src.at[pl.ds(k * step, step)], out.at[pl.ds(k * step, step)], sem.at[k]) for k in range(8)]
    for c in cs:
        c.start()
    for c in cs:
        c.wait()


def solution(mesh):
    vmem = pl.BlockSpec(memory_space=pltpu.VMEM)
    hbm = pl.BlockSpec(memory_space=pltpu.HBM)
    dma = pltpu.SemaphoreType.DMA

    def device_step(hidden, w_gate, w_up, w_down, norm_gain, w_vocab, temperature, target):
        wide, small = pl.pallas_call(
            _main,
            out_shape=(pltpu.VMEM((B, V), BF16), pltpu.VMEM((8, 128), F32)),
            in_specs=[hbm] * 8,
            out_specs=(vmem, vmem),
            scratch_shapes=[
                pltpu.VMEM((2048, 3072), BF16), pltpu.VMEM((D, VL), BF16), pltpu.VMEM((B, D), BF16),
                pltpu.VMEM((B, FL), BF16), pltpu.VMEM((B, D), F32), pltpu.VMEM((HALF, D), BF16),
                pltpu.VMEM((HALF, D), BF16), pltpu.VMEM((HALF, D), BF16), pltpu.VMEM((3 * PIECE, D), BF16),
                pltpu.VMEM((B, D), BF16), pltpu.VMEM((128, 128), F32), pltpu.VMEM((128, 128), F32),
                pltpu.VMEM((128, 128), F32), pltpu.VMEM((128, 128), F32), pltpu.VMEM((128, 128), jnp.int32),
                pltpu.VMEM((1, D), F32), pltpu.VMEM((1, B), F32), pltpu.VMEM((1, B), jnp.int32),
                dma((4,)), dma((NF,)), dma((NJ,)), dma((NW,)),
                dma, dma((NJ,)), dma, dma, dma, dma((3,)), dma, dma, dma, dma,
                dma((NC,)), dma((NC + (NC - SPLIT) * (NS - 1),)), dma((NC,)), dma((NC + (NC - SPLIT) * (NS - 1),)),
            ],
            compiler_params=pltpu.CompilerParams(collective_id=0, has_side_effects=True, vmem_limit_bytes=49 << 20),
            name="step",
        )(hidden, w_gate, w_up, w_down, norm_gain.reshape(1, D), w_vocab, temperature.reshape(1, B), target.reshape(1, B))
        row = jax.ShapeDtypeStruct((1, B), F32)
        log_probs, log_norm, entropy, target_logp = pl.pallas_call(
            _write,
            out_shape=(jax.ShapeDtypeStruct((B, V), BF16), row, row, row),
            in_specs=[vmem, vmem],
            out_specs=(hbm, hbm, hbm, hbm),
            scratch_shapes=[dma((11,))],
            compiler_params=pltpu.CompilerParams(vmem_limit_bytes=16 << 20),
            name="write",
        )(wide, small)
        return log_norm.reshape(B), entropy.reshape(B), target_logp.reshape(B), log_probs

    return jax.shard_map(
        device_step,
        mesh=mesh,
        in_specs=(P("dp", None), P(None, "tp"), P(None, "tp"), P("tp", None), P(None),
                  P(None, "tp"), P("dp"), P("dp")),
        out_specs=(P("dp"), P("dp"), P("dp"), P("dp", None)),
        check_vma=False,
    )
```

```python
import jax
import jax.numpy as jnp
from jax import lax
from jax.experimental import pallas as pl
from jax.experimental.pallas import tpu as pltpu
from jax.sharding import PartitionSpec as P

NORM_EPS = 1e-6
F32 = jnp.float32
BF16 = jnp.bfloat16
B, D, FL, V, VL = 128, 2048, 1024, 49152, 6144
NC = 8
CW = VL // NC
GRID = 3072 // CW
EARLY = 3
OWN = 6
SPLIT = 6
CUTS = (0, 4, 7, 8)
NS = len(CUTS) - 1
NF = 4
FW = FL // NF
NJ = 4
JW = D // NJ
HALF, PIECE = 64, 16
NW = 4
WW = VL // NW


ORDER = (0, 2, 4, 6, 1, 3, 5, 7)
POS = tuple(ORDER.index(k) for k in range(8))


def _lanes(row):
    return jnp.transpose(jnp.broadcast_to(row, (128, 128)))


def _main(hid_hbm, wg_hbm, wu_hbm, wd_hbm, gain_hbm, wv_hbm, temp_hbm, tgt_hbm,
          out, small,
          w, wv, hid, act, yf, ysend, yrecv, psend, precv, xbuf, statm, stats, offs, invt, tgtm, gain, temp, tgt,
          in_sem, wf_sem, wd_sem, wv_sem,
          d2d_s, d2d_r, rs_s, rs_r, x_s, xa_r, xf_r, st_s, st_r, bulk_s, rxy, rd, pr, prd):
    me = lax.axis_index("tp")
    core = me % 2
    nx, ny, nd, pt = me ^ 2, me ^ 4, me ^ 6, me ^ 1

    def remote(src, dst, ss, rs, dev):
        return pltpu.make_async_remote_copy(src, dst, ss, rs, device_id={"tp": dev})

    def load(src, dst, sem):
        c = pltpu.make_async_copy(src, dst, sem)
        c.start()
        return c

    def load_wf(b):
        for t, ref in enumerate((wg_hbm, wu_hbm)):
            load(ref.at[:, pl.ds(b * FW, FW)], w.at[:, pl.ds(t * FL + b * FW, FW)], wf_sem.at[b])

    def wait_wf(b):
        both = w.at[:, pl.ds(0, 2 * FW)]
        pltpu.make_async_copy(wv_hbm.at[:, pl.ds(0, 2 * FW)], both, wf_sem.at[b]).wait()

    def load_wd(j):
        return load(wd_hbm.at[:, pl.ds(j * JW, JW)], w.at[pl.ds(j % 2 * FL, FL), pl.ds(2 * FL + j // 2 * JW, JW)], wd_sem.at[j])

    def load_wv(n):
        return load(wv_hbm.at[:, pl.ds(n * WW, WW)], wv.at[:, pl.ds(n * WW, WW)], wv_sem.at[n])

    hid_copy = load(hid_hbm, hid, in_sem.at[0])
    load_wf(0)
    small_copies = [load(temp_hbm, temp, in_sem.at[1]), load(tgt_hbm, tgt, in_sem.at[2]), load(gain_hbm, gain, in_sem.at[3])]
    load_wf(1)

    barrier = pltpu.get_barrier_semaphore()
    for k in range(1, 8):
        pl.semaphore_signal(barrier, inc=1, device_id={"tp": me ^ k})

    hid_copy.wait()
    wd_copies, wv_copies = [], []
    for b in range(NF):
        wait_wf(b)
        if b < NF - 2:
            load_wf(b + 2)
        else:
            for j in range((b - NF + 2) * NJ // 2, (b - NF + 3) * NJ // 2):
                wd_copies.append(load_wd(j))
            if b == NF - 1:
                wv_copies.append(load_wv(0))
        g = jnp.dot(hid[...], w[:, b * FW:(b + 1) * FW], preferred_element_type=F32)
        u = jnp.dot(hid[...], w[:, FL + b * FW:FL + (b + 1) * FW], preferred_element_type=F32)
        act[:, b * FW:(b + 1) * FW] = (jax.nn.silu(g) * u).astype(BF16)

    keep = pl.multiple_of(core * HALF, HALF)
    give = pl.multiple_of(HALF - core * HALF, HALF)
    d2d = []
    for j in range(NJ):
        cols = pl.ds(j * JW, JW)
        wd_copies[j].wait()
        if j < NW - 1:
            wv_copies.append(load_wv(j + 1))
        wd = w[j % 2 * FL:(j % 2 + 1) * FL, 2 * FL + j // 2 * JW:2 * FL + (j // 2 + 1) * JW]
        yf[:, j * JW:(j + 1) * JW] = jnp.dot(act[...], wd, preferred_element_type=F32)
        ysend[:, j * JW:(j + 1) * JW] = yf[pl.ds(give, HALF), j * JW:(j + 1) * JW].astype(BF16)
        if j == 0:
            pl.semaphore_wait(barrier, 7)
        c = remote(ysend.at[:, cols], yrecv.at[:, cols], d2d_s, d2d_r.at[j], pt)
        c.start()
        d2d.append(c)

    def rows_of(dev):
        return pl.multiple_of((dev % 2) * HALF + (dev // 2) * PIECE, PIECE)

    for n in range(min(NJ + 1, NW), NW):
        wv_copies.append(load_wv(n))
    for c in small_copies:
        c.wait()
    offs[...] = _lanes(1.0 / temp[...])
    statm[...] = _lanes(tgt[...].astype(F32))
    for p, k in enumerate(ORDER):
        rows = pl.ds(rows_of(me ^ k), PIECE)
        invt[p * PIECE:(p + 1) * PIECE, :] = offs[rows, :]
        tgtm[p * PIECE:(p + 1) * PIECE, :] = statm[rows, :].astype(jnp.int32)

    def piece(dev):
        return pl.multiple_of((dev // 2) * PIECE, PIECE)

    for j in range(NJ):
        cols = slice(j * JW, (j + 1) * JW)
        d2d[j].wait_recv()
        part = yf[pl.ds(keep, HALF), cols] + yrecv[:, cols].astype(F32)
        yf[pl.ds(keep, HALF), cols] = part
        psend[:, cols] = part.astype(BF16)
        for s, dev in enumerate((nd, nx, ny)):
            remote(psend.at[pl.ds(piece(dev), PIECE), pl.ds(j * JW, JW)], precv.at[pl.ds(s * PIECE, PIECE), pl.ds(j * JW, JW)],
                   rs_s, rs_r, dev).start()
    rs_all = remote(precv, precv, rs_s, rs_r, nx)
    rs_all.wait_recv()
    mine = rows_of(me)
    y = yf[pl.ds(mine, PIECE), :]
    for s in range(3):
        y = y + precv[s * PIECE:(s + 1) * PIECE, :].astype(F32)
    res = hid[pl.ds(mine, PIECE), :].astype(F32) + y
    inv_rms = lax.rsqrt(jnp.mean(res * res, axis=-1, keepdims=True) + NORM_EPS)
    xbuf[0:PIECE, :] = (gain[...] * res * inv_rms).astype(BF16)

    def xrow(k):
        return xbuf.at[pl.ds(POS[k] * PIECE, PIECE), :]

    for s, k in enumerate((6, 2, 4)):
        remote(xrow(0), xrow(k), x_s, xa_r.at[s], me ^ k).start()
    remote(xrow(0), xrow(1), x_s, xf_r, pt).start()

    def place(dev, i):
        row = pl.multiple_of((dev * 2 + i // GRID) * 128, 128)
        col = pl.multiple_of((i % GRID) * CW, CW)
        return row, pl.ds(col, CW)

    def chunk(dev, i):
        row, cols = place(dev, i)
        return w.at[pl.ds(row, 128), cols]

    def own_start(i, first, count):
        row, cols = place(me, i)
        ref = w.at[pl.ds(row + first, count), cols]
        remote(ref, ref, bulk_s, rxy.at[i], nx).start()
        remote(ref, ref, bulk_s, rxy.at[i], ny).start()
        remote(ref, ref, bulk_s, pr.at[i], pt).start()

    def head(i, first, count, go=False):
        acc = jnp.dot(xbuf[first:first + count, :], wv[:, pl.ds(pl.multiple_of(i * CW, CW), CW)], preferred_element_type=F32)
        scale = invt[first:first + count, :]
        parts = [acc[:, q * 128:(q + 1) * 128] * scale for q in range(CW // 128)]
        top = parts[0]
        for p in parts[1:]:
            top = jnp.maximum(top, p)
        top = jnp.max(top, axis=-1, keepdims=True)
        row, _ = place(me, i)
        for q, p in enumerate(parts):
            w[pl.ds(row + first, count), pl.ds(pl.multiple_of((i % GRID) * CW + q * 128, 128), 128)] = (p - top).astype(BF16)
        if go:
            own_start(i, first, count)
        elif first:
            @pl.when(i < EARLY)
            def _():
                own_start(i, first, count)

        total = weighted = hit = jnp.zeros((count, 128), F32)
        lane = lax.broadcasted_iota(jnp.int32, (count, 128), 1)
        ids = tgtm[first:first + count, :] - (me * VL + i * CW)
        for q, p in enumerate(parts):
            e = jnp.exp(p - top)
            total = total + e
            weighted = weighted + e * p
            hit = hit + jnp.where(ids == lane + q * 128, p, 0.0)
        sm = statm[first:first + count, :]
        sm = jnp.where(lane == i, top, sm)
        sm = jnp.where(lane == 16 + i, jnp.sum(total, axis=-1, keepdims=True), sm)
        sm = jnp.where(lane == 32 + i, jnp.sum(weighted, axis=-1, keepdims=True), sm)
        sm = jnp.where(lane == 48 + i, jnp.sum(hit, axis=-1, keepdims=True), sm)
        statm[first:first + count, :] = sm

    def head_own(i, _):
        head(i, 0, PIECE, True)
        return 0

    def head_rest(i, _):
        head(i, PIECE, B - PIECE)
        return 0

    def head_all(i, _):
        head(i, 0, B)
        return 0

    ready = 0
    for i in range(OWN):
        while ready * WW < (i + 1) * CW:
            wv_copies[ready].wait()
            ready += 1
        head_own(i, 0)
    for s, k in ((1, 2), (2, 4), (0, 6)):
        remote(xrow(k), xrow(k), x_s, xa_r.at[s], me ^ k).wait_recv()
        remote(xrow(k), xrow(k + 1), x_s, xf_r, pt).start()
    head(0, PIECE, HALF - PIECE, True)
    four = xbuf.at[pl.ds(0, 4 * PIECE), :]
    remote(four, four, x_s, xf_r, pt).wait_recv()
    head(0, HALF, HALF, True)
    for c in wv_copies[ready:]:
        c.wait()
    lax.fori_loop(1, OWN, head_rest, 0)
    lax.fori_loop(OWN, NC, head_all, 0)

    for p, k in enumerate(ORDER):
        offs[pl.ds(rows_of(me ^ k), PIECE), :] = statm[p * PIECE:(p + 1) * PIECE, :]
    st = jnp.transpose(offs[...])
    tops = st[0:NC, :]
    top = jnp.max(tops, axis=0, keepdims=True)
    scale = jnp.exp(tops - top)
    my_stats = jnp.concatenate(
        [tops, top, jnp.sum(scale * st[16:16 + NC, :], axis=0, keepdims=True),
         jnp.sum(scale * st[32:32 + NC, :], axis=0, keepdims=True),
         jnp.sum(st[48:48 + NC, :], axis=0, keepdims=True),
         jnp.zeros((16 - NC - 4, 128), F32)], axis=0)

    stats[0:16, :] = my_stats
    for k in range(1, 8):
        remote(stats.at[pl.ds(0, 16), :], stats.at[pl.ds(16 * k, 16), :], st_s, st_r, me ^ k).start()

    def send_rest(i, _):
        own_start(i, PIECE, B - PIECE)
        return 0

    def send_all(i, _):
        own_start(i, 0, B)
        return 0

    lax.fori_loop(EARLY, OWN, send_rest, 0)
    lax.fori_loop(OWN, NC, send_all, 0)

    others = stats.at[pl.ds(16, 112), :]
    st_all = remote(others, others, st_s, st_r, nx)
    st_all.wait_recv()
    allst = [stats[16 * k:16 * (k + 1), :] for k in range(8)]
    top = allst[0][NC:NC + 1, :]
    for s in allst[1:]:
        top = jnp.maximum(top, s[NC:NC + 1, :])
    total = weighted = hit = jnp.zeros((1, 128), F32)
    for s in allst:
        scale = jnp.exp(s[NC:NC + 1, :] - top)
        total = total + scale * s[NC + 1:NC + 2, :]
        weighted = weighted + scale * s[NC + 2:NC + 3, :]
        hit = hit + s[NC + 3:NC + 4, :]
    log_norm = top + jnp.log(total)
    small[0:1, :] = log_norm
    small[1:2, :] = log_norm - weighted / total
    small[2:3, :] = hit - log_norm
    small[3:8, :] = jnp.zeros((5, 128), F32)
    offs[...] = jnp.transpose(stats[...] - log_norm)

    lane16 = lax.broadcasted_iota(jnp.int32, (PIECE, 128), 1)

    def fix(rel, i, first=0, count=8):
        dev = me ^ rel
        row, cols = place(dev, i)
        for k in range(first, first + count):
            rows = pl.ds(rows_of(dev ^ ORDER[k]), PIECE)
            off = jnp.sum(jnp.where(lane16 == rel * 16 + i, offs[rows, :], 0.0), axis=-1, keepdims=True)
            val = w[pl.ds(row + k * PIECE, PIECE), cols].astype(F32) + off
            out[rows, pl.ds(pl.multiple_of(dev * VL + i * CW, CW), CW)] = val.astype(BF16)

    def land(n):
        return w.at[pl.ds(0, n * 128), pl.ds(0, CW)]

    def arrived(n, sem):
        remote(land(n), land(n), bulk_s, sem, nx).wait_recv()

    def forward(rel, i, sem, to):
        ref = chunk(me ^ rel, i)
        remote(ref, ref, bulk_s, sem, to).start()

    def pieces(rel, i, n):
        row, cols = place(me ^ rel, i)
        return w.at[pl.ds(row + CUTS[n] * PIECE, (CUTS[n + 1] - CUTS[n]) * PIECE), cols]

    def piece_sem(sems, i, n):
        return sems.at[i if n == 0 else NC + (i - SPLIT) * (NS - 1) + n - 1]

    def relay(rel, i, to):
        if isinstance(i, int):
            for n in range(NS):
                ref = pieces(rel, i, n)
                remote(ref, ref, bulk_s, piece_sem(rd, i, n), to).start()
            remote(ref, ref, bulk_s, piece_sem(prd, i, NS - 1), to ^ 1).start()
        else:
            forward(rel, i, rd.at[i], to)

    def arrivals(i, _):
        arrived(2, rxy.at[i])
        if isinstance(i, int):
            relay(2, i, ny) if i % 2 == 0 else relay(4, i, nx)
        else:
            @pl.when(i % 2 == 0)
            def _():
                relay(2, i, ny)

            @pl.when(i % 2 == 1)
            def _():
                relay(4, i, nx)

        forward(2, i, pr.at[i], pt)
        forward(4, i, pr.at[i], pt)
        fix(0, i)
        fix(2, i)
        fix(4, i)
        arrived(3, pr.at[i])
        fix(1, i)
        fix(3, i)
        fix(5, i)
        return 0

    lax.fori_loop(0, SPLIT, arrivals, 0)
    for i in range(SPLIT, NC):
        arrivals(i, 0)

    def diagonal(i, _):
        arrived(1, rd.at[i])
        forward(6, i, prd.at[i], pt)
        fix(6, i)
        arrived(1, prd.at[i])
        fix(7, i)
        return 0

    lax.fori_loop(0, SPLIT, diagonal, 0)
    def part(n):
        return w.at[pl.ds(0, (CUTS[n + 1] - CUTS[n]) * PIECE), pl.ds(0, CW)]

    for n in range(NS):
        for i in range(SPLIT, NC):
            remote(part(n), part(n), bulk_s, piece_sem(rd, i, n), nx).wait_recv()
            if n < NS - 1:
                ref = pieces(6, i, n)
                remote(ref, ref, bulk_s, piece_sem(prd, i, n), pt).start()
            fix(6, i, CUTS[n], CUTS[n + 1] - CUTS[n])
    for n in range(NS):
        for i in range(SPLIT, NC):
            remote(part(n), part(n), bulk_s, piece_sem(prd, i, n), pt).wait_recv()
            fix(7, i, CUTS[n], CUTS[n + 1] - CUTS[n])

    def left(ref, sem):
        remote(ref, ref, sem, rs_r, nx).wait_send()

    left(ysend, d2d_s)
    rs_all.wait_send()
    left(xbuf.at[pl.ds(0, 7 * PIECE), :], x_s)
    st_all.wait_send()
    left(w.at[pl.ds(0, 1792), :], bulk_s)


def _write(src, small, out, o0, o1, o2, sem):
    step = B // 16
    cs = [pltpu.make_async_copy(small.at[pl.ds(k, 1), :], o, sem.at[k]) for k, o in enumerate((o0, o1, o2))]
    for k in range(16):
        pltpu.make_async_copy(src.at[pl.ds(k * step, step)], out.at[pl.ds(k * step, step)], sem.at[3]).start()
    for c in cs:
        c.start()
    for c in cs:
        c.wait()
    pltpu.make_async_copy(src, out, sem.at[3]).wait()


def solution(mesh):
    vmem = pl.BlockSpec(memory_space=pltpu.VMEM)
    hbm = pl.BlockSpec(memory_space=pltpu.HBM)
    dma = pltpu.SemaphoreType.DMA

    def device_step(hidden, w_gate, w_up, w_down, norm_gain, w_vocab, temperature, target):
        wide, small = pl.pallas_call(
            _main,
            out_shape=(pltpu.VMEM((B, V), BF16), pltpu.VMEM((8, 128), F32)),
            in_specs=[hbm] * 8,
            out_specs=(vmem, vmem),
            scratch_shapes=[
                pltpu.VMEM((2048, 3072), BF16), pltpu.VMEM((D, VL), BF16), pltpu.VMEM((B, D), BF16),
                pltpu.VMEM((B, FL), BF16), pltpu.VMEM((B, D), F32), pltpu.VMEM((HALF, D), BF16),
                pltpu.VMEM((HALF, D), BF16), pltpu.VMEM((HALF, D), BF16), pltpu.VMEM((3 * PIECE, D), BF16),
                pltpu.VMEM((B, D), BF16), pltpu.VMEM((128, 128), F32), pltpu.VMEM((128, 128), F32),
                pltpu.VMEM((128, 128), F32), pltpu.VMEM((128, 128), F32), pltpu.VMEM((128, 128), jnp.int32),
                pltpu.VMEM((1, D), F32), pltpu.VMEM((1, B), F32), pltpu.VMEM((1, B), jnp.int32),
                dma((4,)), dma((NF,)), dma((NJ,)), dma((NW,)),
                dma, dma((NJ,)), dma, dma, dma, dma((3,)), dma, dma, dma, dma,
                dma((NC,)), dma((NC + (NC - SPLIT) * (NS - 1),)), dma((NC,)), dma((NC + (NC - SPLIT) * (NS - 1),)),
            ],
            compiler_params=pltpu.CompilerParams(collective_id=0, has_side_effects=True, vmem_limit_bytes=49 << 20),
            name="step",
        )(hidden, w_gate, w_up, w_down, norm_gain.reshape(1, D), w_vocab, temperature.reshape(1, B), target.reshape(1, B))
        row = jax.ShapeDtypeStruct((1, B), F32)
        log_probs, log_norm, entropy, target_logp = pl.pallas_call(
            _write,
            out_shape=(jax.ShapeDtypeStruct((B, V), BF16), row, row, row),
            in_specs=[vmem, vmem],
            out_specs=(hbm, hbm, hbm, hbm),
            scratch_shapes=[dma((4,))],
            compiler_params=pltpu.CompilerParams(vmem_limit_bytes=16 << 20),
            name="write",
        )(wide, small)
        return log_norm.reshape(B), entropy.reshape(B), target_logp.reshape(B), log_probs

    return jax.shard_map(
        device_step,
        mesh=mesh,
        in_specs=(P("dp", None), P(None, "tp"), P(None, "tp"), P("tp", None), P(None),
                  P(None, "tp"), P("dp"), P("dp")),
        out_specs=(P("dp"), P("dp"), P("dp"), P("dp", None)),
        check_vma=False,
    )
```

```python
import jax
import jax.numpy as jnp
from jax import lax
from jax.experimental import pallas as pl
from jax.experimental.pallas import tpu as pltpu
from jax.sharding import PartitionSpec as P

NORM_EPS = 1e-6
F32 = jnp.float32
BF16 = jnp.bfloat16
B, D, FL, V, VL = 128, 2048, 1024, 49152, 6144
NC = 8
CW = VL // NC
GRID = 3072 // CW
EARLY = 3
OWN = 7
GROUP = 2
SPLIT = 6
CUTS = (0, 4, 7, 8)
NS = len(CUTS) - 1
NF = 4
FW = FL // NF
NJ = 4
JW = D // NJ
HALF, PIECE = 64, 16
NW = 4
WW = VL // NW


ORDER = (0, 2, 4, 6, 1, 3, 5, 7)
POS = tuple(ORDER.index(k) for k in range(8))


def _lanes(row):
    return jnp.transpose(jnp.broadcast_to(row, (128, 128)))


def _main(hid_hbm, wg_hbm, wu_hbm, wd_hbm, gain_hbm, wv_hbm, temp_hbm, tgt_hbm,
          out, small,
          w, wv, hid, act, yf, yall, ysend, yrecv, psend, precv0, precv, xbuf, kept, statm, stats, offs, invt, tgtm, gain, temp, tgt,
          in_sem, wf_sem, wd_sem, wv_sem,
          d2d_s, d2d_r, rs_s, rs_r, x_s, xa_r, xf_r, st_s, st_r, bulk_s, rxy, rd, pr, prd):
    me = lax.axis_index("tp")
    core = me % 2
    nx, ny, nd, pt = me ^ 2, me ^ 4, me ^ 6, me ^ 1

    def remote(src, dst, ss, rs, dev):
        return pltpu.make_async_remote_copy(src, dst, ss, rs, device_id={"tp": dev})

    def load(src, dst, sem):
        c = pltpu.make_async_copy(src, dst, sem)
        c.start()
        return c

    def load_wf(b):
        for t, ref in enumerate((wg_hbm, wu_hbm)):
            load(ref.at[:, pl.ds(b * FW, FW)], w.at[:, pl.ds(t * FL + b * FW, FW)], wf_sem.at[b])

    def wait_wf(b):
        both = w.at[:, pl.ds(0, 2 * FW)]
        pltpu.make_async_copy(wv_hbm.at[:, pl.ds(0, 2 * FW)], both, wf_sem.at[b]).wait()

    def load_wd(j):
        return load(wd_hbm.at[:, pl.ds(j * JW, JW)], w.at[pl.ds(j % 2 * FL, FL), pl.ds(2 * FL + j // 2 * JW, JW)], wd_sem.at[j])

    def load_wv(n):
        return load(wv_hbm.at[:, pl.ds(n * WW, WW)], wv.at[:, pl.ds(n * WW, WW)], wv_sem.at[n])

    hid_copy = load(hid_hbm, hid, in_sem.at[0])
    load_wf(0)
    small_copies = [load(temp_hbm, temp, in_sem.at[1]), load(tgt_hbm, tgt, in_sem.at[2]), load(gain_hbm, gain, in_sem.at[3])]
    load_wf(1)

    barrier = pltpu.get_barrier_semaphore()
    for k in range(1, 8):
        pl.semaphore_signal(barrier, inc=1, device_id={"tp": me ^ k})

    hid_copy.wait()
    wd_copies, wv_copies = [], []
    for b in range(NF):
        wait_wf(b)
        if b < NF - 2:
            load_wf(b + 2)
        else:
            for j in range((b - NF + 2) * NJ // 2, (b - NF + 3) * NJ // 2):
                wd_copies.append(load_wd(j))
            if b == NF - 1:
                wv_copies.append(load_wv(0))
        g = jnp.dot(hid[...], w[:, b * FW:(b + 1) * FW], preferred_element_type=F32)
        u = jnp.dot(hid[...], w[:, FL + b * FW:FL + (b + 1) * FW], preferred_element_type=F32)
        act[:, b * FW:(b + 1) * FW] = (jax.nn.silu(g) * u).astype(BF16)

    def rows_of(dev):
        return pl.multiple_of((dev % 2) * HALF + (dev // 2) * PIECE, PIECE)

    keep = pl.multiple_of(core * HALF, HALF)
    give = pl.multiple_of(HALF - core * HALF, HALF)
    d2d = []
    for j in range(NJ):
        wd_copies[j].wait()
        if j < NW - 1:
            wv_copies.append(load_wv(j + 1))
        wd = w[j % 2 * FL:(j % 2 + 1) * FL, 2 * FL + j // 2 * JW:2 * FL + (j // 2 + 1) * JW]
        yf[:, j * JW:(j + 1) * JW] = jnp.dot(act[...], wd, preferred_element_type=F32)
        if j == 0:
            yall[...] = yf[:, 0:JW].astype(BF16)
            pl.semaphore_wait(barrier, 7)
            for k in (6, 7, 2, 3, 4, 5, 1):
                remote(yall.at[pl.ds(rows_of(me ^ k), PIECE), :], precv0.at[pl.ds((k - 1) * PIECE, PIECE), :],
                       rs_s, rs_r, me ^ k).start()
            continue
        ysend[:, (j - 1) * JW:j * JW] = yf[pl.ds(give, HALF), j * JW:(j + 1) * JW].astype(BF16)
        cols = pl.ds((j - 1) * JW, JW)
        c = remote(ysend.at[:, cols], yrecv.at[:, cols], d2d_s, d2d_r.at[j - 1], pt)
        c.start()
        d2d.append(c)

    for n in range(min(NJ + 1, NW), NW):
        wv_copies.append(load_wv(n))
    for c in small_copies:
        c.wait()
    offs[...] = _lanes(1.0 / temp[...])
    statm[...] = _lanes(tgt[...].astype(F32))
    for p, k in enumerate(ORDER):
        rows = pl.ds(rows_of(me ^ k), PIECE)
        invt[p * PIECE:(p + 1) * PIECE, :] = offs[rows, :]
        tgtm[p * PIECE:(p + 1) * PIECE, :] = statm[rows, :].astype(jnp.int32)

    def piece(dev):
        return pl.multiple_of((dev // 2) * PIECE, PIECE)

    for j in range(1, NJ):
        cols = slice(j * JW, (j + 1) * JW)
        got = pl.ds((j - 1) * JW, JW)
        d2d[j - 1].wait_recv()
        part = yf[pl.ds(keep, HALF), cols] + yrecv[:, (j - 1) * JW:j * JW].astype(F32)
        yf[pl.ds(keep, HALF), cols] = part
        psend[:, (j - 1) * JW:j * JW] = part.astype(BF16)
        for s, dev in enumerate((nd, nx, ny)):
            remote(psend.at[pl.ds(piece(dev), PIECE), got], precv.at[pl.ds(s * PIECE, PIECE), got], rs_s, rs_r, dev).start()

    rs_all = remote(hid.at[pl.ds(0, HALF), :], hid.at[pl.ds(0, HALF), :], rs_s, rs_r, nx)
    rs_all.wait_recv()
    mine = rows_of(me)
    y0 = yf[pl.ds(mine, PIECE), 0:JW]
    for k in range(7):
        y0 = y0 + precv0[k * PIECE:(k + 1) * PIECE, :].astype(F32)
    y1 = yf[pl.ds(mine, PIECE), JW:D]
    for s in range(3):
        y1 = y1 + precv[s * PIECE:(s + 1) * PIECE, :].astype(F32)
    y = jnp.concatenate([y0, y1], axis=-1)
    res = hid[pl.ds(mine, PIECE), :].astype(F32) + y
    inv_rms = lax.rsqrt(jnp.mean(res * res, axis=-1, keepdims=True) + NORM_EPS)
    xbuf[0:PIECE, :] = (gain[...] * res * inv_rms).astype(BF16)

    def xrow(k):
        return xbuf.at[pl.ds(POS[k] * PIECE, PIECE), :]

    for s, k in enumerate((6, 2, 4)):
        remote(xrow(0), xrow(k), x_s, xa_r.at[s], me ^ k).start()
    remote(xrow(0), xrow(1), x_s, xf_r, pt).start()

    def place(dev, i):
        row = pl.multiple_of((dev * 2 + i // GRID) * 128, 128)
        col = pl.multiple_of((i % GRID) * CW, CW)
        return row, pl.ds(col, CW)

    def chunk(dev, i):
        row, cols = place(dev, i)
        return w.at[pl.ds(row, 128), cols]

    def own_start(i, first, count):
        row, cols = place(me, i)
        ref = w.at[pl.ds(row + first, count), cols]
        remote(ref, ref, bulk_s, rxy.at[i], nx).start()
        remote(ref, ref, bulk_s, rxy.at[i], ny).start()
        remote(ref, ref, bulk_s, pr.at[i], pt).start()

    def logits(i, first, count):
        acc = jnp.dot(xbuf[first:first + count, :], wv[:, pl.ds(pl.multiple_of(i * CW, CW), CW)], preferred_element_type=F32)
        scale = invt[first:first + count, :]
        return [acc[:, q * 128:(q + 1) * 128] * scale for q in range(CW // 128)]

    def row_max(parts):
        top = parts[0]
        for p in parts[1:]:
            top = jnp.maximum(top, p)
        return jnp.max(top, axis=-1, keepdims=True)

    def put(i, first, count, parts, top):
        row, _ = place(me, i)
        for q, p in enumerate(parts):
            w[pl.ds(row + first, count), pl.ds(pl.multiple_of((i % GRID) * CW + q * 128, 128), 128)] = (p - top).astype(BF16)

    def statistics(i, first, count, parts, top):
        total = weighted = hit = jnp.zeros((count, 128), F32)
        lane = lax.broadcasted_iota(jnp.int32, (count, 128), 1)
        ids = tgtm[first:first + count, :] - (me * VL + i * CW)
        for q, p in enumerate(parts):
            e = jnp.exp(p - top)
            total = total + e
            weighted = weighted + e * p
            hit = hit + jnp.where(ids == lane + q * 128, p, 0.0)
        sm = statm[first:first + count, :]
        sm = jnp.where(lane == i, top, sm)
        sm = jnp.where(lane == 16 + i, jnp.sum(total, axis=-1, keepdims=True), sm)
        sm = jnp.where(lane == 32 + i, jnp.sum(weighted, axis=-1, keepdims=True), sm)
        sm = jnp.where(lane == 48 + i, jnp.sum(hit, axis=-1, keepdims=True), sm)
        statm[first:first + count, :] = sm

    def head(i, first, count, go=False):
        parts = logits(i, first, count)
        top = row_max(parts)
        put(i, first, count, parts, top)
        if go:
            own_start(i, first, count)
        elif first:
            @pl.when(i < EARLY)
            def _():
                own_start(i, first, count)

        statistics(i, first, count, parts, top)

    def head_rest(i, _):
        head(i, PIECE, B - PIECE)
        return 0

    def head_all(i, _):
        head(i, 0, B)
        return 0

    def own_statistics(i, _):
        parts = [kept[:, pl.ds(pl.multiple_of(i * CW + q * 128, 128), 128)] for q in range(CW // 128)]
        statistics(i, 0, PIECE, parts, row_max(parts))
        return 0

    ready = 0
    for start in range(0, OWN, GROUP):
        group = range(start, min(start + GROUP, OWN))
        while ready * WW < (group[-1] + 1) * CW:
            wv_copies[ready].wait()
            ready += 1
        block = [logits(i, 0, PIECE) for i in group]
        for i, parts in zip(group, block):
            put(i, 0, PIECE, parts, row_max(parts))
            for q, p in enumerate(parts):
                kept[:, i * CW + q * 128:i * CW + (q + 1) * 128] = p
        for i in group:
            own_start(i, 0, PIECE)
    for s, k in ((1, 2), (2, 4), (0, 6)):
        remote(xrow(k), xrow(k), x_s, xa_r.at[s], me ^ k).wait_recv()
        remote(xrow(k), xrow(k + 1), x_s, xf_r, pt).start()
    head(0, PIECE, HALF - PIECE, True)
    four = xbuf.at[pl.ds(0, 4 * PIECE), :]
    remote(four, four, x_s, xf_r, pt).wait_recv()
    head(0, HALF, HALF, True)
    for c in wv_copies[ready:]:
        c.wait()
    lax.fori_loop(1, OWN, head_rest, 0)
    lax.fori_loop(OWN, NC, head_all, 0)
    lax.fori_loop(0, OWN, own_statistics, 0)

    for p, k in enumerate(ORDER):
        offs[pl.ds(rows_of(me ^ k), PIECE), :] = statm[p * PIECE:(p + 1) * PIECE, :]
    st = jnp.transpose(offs[...])
    tops = st[0:NC, :]
    top = jnp.max(tops, axis=0, keepdims=True)
    scale = jnp.exp(tops - top)
    my_stats = jnp.concatenate(
        [tops, top, jnp.sum(scale * st[16:16 + NC, :], axis=0, keepdims=True),
         jnp.sum(scale * st[32:32 + NC, :], axis=0, keepdims=True),
         jnp.sum(st[48:48 + NC, :], axis=0, keepdims=True),
         jnp.zeros((16 - NC - 4, 128), F32)], axis=0)

    stats[0:16, :] = my_stats
    for k in range(1, 8):
        remote(stats.at[pl.ds(0, 16), :], stats.at[pl.ds(16 * k, 16), :], st_s, st_r, me ^ k).start()

    def send_rest(i, _):
        own_start(i, PIECE, B - PIECE)
        return 0

    def send_all(i, _):
        own_start(i, 0, B)
        return 0

    lax.fori_loop(EARLY, OWN, send_rest, 0)
    lax.fori_loop(OWN, NC, send_all, 0)

    others = stats.at[pl.ds(16, 112), :]
    st_all = remote(others, others, st_s, st_r, nx)
    st_all.wait_recv()
    allst = [stats[16 * k:16 * (k + 1), :] for k in range(8)]
    top = allst[0][NC:NC + 1, :]
    for s in allst[1:]:
        top = jnp.maximum(top, s[NC:NC + 1, :])
    total = weighted = hit = jnp.zeros((1, 128), F32)
    for s in allst:
        scale = jnp.exp(s[NC:NC + 1, :] - top)
        total = total + scale * s[NC + 1:NC + 2, :]
        weighted = weighted + scale * s[NC + 2:NC + 3, :]
        hit = hit + s[NC + 3:NC + 4, :]
    log_norm = top + jnp.log(total)
    small[0:1, :] = log_norm
    small[1:2, :] = log_norm - weighted / total
    small[2:3, :] = hit - log_norm
    small[3:8, :] = jnp.zeros((5, 128), F32)
    offs[...] = jnp.transpose(stats[...] - log_norm)

    lane16 = lax.broadcasted_iota(jnp.int32, (PIECE, 128), 1)

    def fix(rel, i, first=0, count=8):
        dev = me ^ rel
        row, cols = place(dev, i)
        for k in range(first, first + count):
            rows = pl.ds(rows_of(dev ^ ORDER[k]), PIECE)
            off = jnp.sum(jnp.where(lane16 == rel * 16 + i, offs[rows, :], 0.0), axis=-1, keepdims=True)
            val = w[pl.ds(row + k * PIECE, PIECE), cols].astype(F32) + off
            out[rows, pl.ds(pl.multiple_of(dev * VL + i * CW, CW), CW)] = val.astype(BF16)

    def land(n):
        return w.at[pl.ds(0, n * 128), pl.ds(0, CW)]

    def arrived(n, sem):
        remote(land(n), land(n), bulk_s, sem, nx).wait_recv()

    def forward(rel, i, sem, to):
        ref = chunk(me ^ rel, i)
        remote(ref, ref, bulk_s, sem, to).start()

    def pieces(rel, i, n):
        row, cols = place(me ^ rel, i)
        return w.at[pl.ds(row + CUTS[n] * PIECE, (CUTS[n + 1] - CUTS[n]) * PIECE), cols]

    def piece_sem(sems, i, n):
        return sems.at[i if n == 0 else NC + (i - SPLIT) * (NS - 1) + n - 1]

    def relay(rel, i, to):
        if isinstance(i, int):
            for n in range(NS):
                ref = pieces(rel, i, n)
                remote(ref, ref, bulk_s, piece_sem(rd, i, n), to).start()
            remote(ref, ref, bulk_s, piece_sem(prd, i, NS - 1), to ^ 1).start()
        else:
            forward(rel, i, rd.at[i], to)

    def arrivals(i, _):
        arrived(2, rxy.at[i])
        if isinstance(i, int):
            relay(2, i, ny) if i % 2 == 0 else relay(4, i, nx)
        else:
            @pl.when(i % 2 == 0)
            def _():
                relay(2, i, ny)

            @pl.when(i % 2 == 1)
            def _():
                relay(4, i, nx)

        forward(2, i, pr.at[i], pt)
        forward(4, i, pr.at[i], pt)
        fix(0, i)
        fix(2, i)
        fix(4, i)
        arrived(3, pr.at[i])
        fix(1, i)
        fix(3, i)
        fix(5, i)
        return 0

    lax.fori_loop(0, SPLIT, arrivals, 0)
    for i in range(SPLIT, NC):
        arrivals(i, 0)

    def diagonal(i, _):
        arrived(1, rd.at[i])
        forward(6, i, prd.at[i], pt)
        fix(6, i)
        arrived(1, prd.at[i])
        fix(7, i)
        return 0

    lax.fori_loop(0, SPLIT, diagonal, 0)
    def part(n):
        return w.at[pl.ds(0, (CUTS[n + 1] - CUTS[n]) * PIECE), pl.ds(0, CW)]

    for n in range(NS):
        for i in range(SPLIT, NC):
            remote(part(n), part(n), bulk_s, piece_sem(rd, i, n), nx).wait_recv()
            if n < NS - 1:
                ref = pieces(6, i, n)
                remote(ref, ref, bulk_s, piece_sem(prd, i, n), pt).start()
            fix(6, i, CUTS[n], CUTS[n + 1] - CUTS[n])
    for n in range(NS):
        for i in range(SPLIT, NC):
            remote(part(n), part(n), bulk_s, piece_sem(prd, i, n), pt).wait_recv()
            fix(7, i, CUTS[n], CUTS[n + 1] - CUTS[n])

    def left(ref, sem):
        remote(ref, ref, sem, rs_r, nx).wait_send()

    left(ysend, d2d_s)
    rs_all.wait_send()
    left(xbuf.at[pl.ds(0, 7 * PIECE), :], x_s)
    st_all.wait_send()
    left(w.at[pl.ds(0, 1792), :], bulk_s)


def _write(src, small, out, o0, o1, o2, sem):
    step = B // 16
    cs = [pltpu.make_async_copy(small.at[pl.ds(k, 1), :], o, sem.at[k]) for k, o in enumerate((o0, o1, o2))]
    for k in range(16):
        pltpu.make_async_copy(src.at[pl.ds(k * step, step)], out.at[pl.ds(k * step, step)], sem.at[3]).start()
    for c in cs:
        c.start()
    for c in cs:
        c.wait()
    pltpu.make_async_copy(src, out, sem.at[3]).wait()


def solution(mesh):
    vmem = pl.BlockSpec(memory_space=pltpu.VMEM)
    hbm = pl.BlockSpec(memory_space=pltpu.HBM)
    dma = pltpu.SemaphoreType.DMA

    def device_step(hidden, w_gate, w_up, w_down, norm_gain, w_vocab, temperature, target):
        wide, small = pl.pallas_call(
            _main,
            out_shape=(pltpu.VMEM((B, V), BF16), pltpu.VMEM((8, 128), F32)),
            in_specs=[hbm] * 8,
            out_specs=(vmem, vmem),
            scratch_shapes=[
                pltpu.VMEM((2048, 3072), BF16), pltpu.VMEM((D, VL), BF16), pltpu.VMEM((B, D), BF16),
                pltpu.VMEM((B, FL), BF16), pltpu.VMEM((B, D), F32), pltpu.VMEM((B, JW), BF16), pltpu.VMEM((HALF, D - JW), BF16),
                pltpu.VMEM((HALF, D - JW), BF16), pltpu.VMEM((HALF, D - JW), BF16), pltpu.VMEM((7 * PIECE, JW), BF16),
                pltpu.VMEM((3 * PIECE, D - JW), BF16),
                pltpu.VMEM((B, D), BF16), pltpu.VMEM((PIECE, OWN * CW), F32), pltpu.VMEM((128, 128), F32), pltpu.VMEM((128, 128), F32),
                pltpu.VMEM((128, 128), F32), pltpu.VMEM((128, 128), F32), pltpu.VMEM((128, 128), jnp.int32),
                pltpu.VMEM((1, D), F32), pltpu.VMEM((1, B), F32), pltpu.VMEM((1, B), jnp.int32),
                dma((4,)), dma((NF,)), dma((NJ,)), dma((NW,)),
                dma, dma((NJ - 1,)), dma, dma, dma, dma((3,)), dma, dma, dma, dma,
                dma((NC,)), dma((NC + (NC - SPLIT) * (NS - 1),)), dma((NC,)), dma((NC + (NC - SPLIT) * (NS - 1),)),
            ],
            compiler_params=pltpu.CompilerParams(collective_id=0, has_side_effects=True, vmem_limit_bytes=49 << 20),
            name="step",
        )(hidden, w_gate, w_up, w_down, norm_gain.reshape(1, D), w_vocab, temperature.reshape(1, B), target.reshape(1, B))
        row = jax.ShapeDtypeStruct((1, B), F32)
        log_probs, log_norm, entropy, target_logp = pl.pallas_call(
            _write,
            out_shape=(jax.ShapeDtypeStruct((B, V), BF16), row, row, row),
            in_specs=[vmem, vmem],
            out_specs=(hbm, hbm, hbm, hbm),
            scratch_shapes=[dma((4,))],
            compiler_params=pltpu.CompilerParams(vmem_limit_bytes=16 << 20),
            name="write",
        )(wide, small)
        return log_norm.reshape(B), entropy.reshape(B), target_logp.reshape(B), log_probs

    return jax.shard_map(
        device_step,
        mesh=mesh,
        in_specs=(P("dp", None), P(None, "tp"), P(None, "tp"), P("tp", None), P(None),
                  P(None, "tp"), P("dp"), P("dp")),
        out_specs=(P("dp"), P("dp"), P("dp"), P("dp", None)),
        check_vma=False,
    )
```

```python
import jax
import jax.numpy as jnp
from jax import lax
from jax.experimental import pallas as pl
from jax.experimental.pallas import tpu as pltpu
from jax.sharding import PartitionSpec as P

NORM_EPS = 1e-6
F32 = jnp.float32
BF16 = jnp.bfloat16
B, D, FL, V, VL = 128, 2048, 1024, 49152, 6144
NC = 8
CW = VL // NC
GRID = 3072 // CW
EARLY = 4
OWN = 7
GROUP = 2
NP = NC // 2
CUTS = (0, 4, 7, 8)
NS = len(CUTS) - 1
NF = 4
FW = FL // NF
NJ = 4
JW = D // NJ
RS_ENDS = (1, 2, 3)
HALF, PIECE = 64, 16
NW = 4
WW = VL // NW


ORDER = (0, 2, 4, 6, 1, 3, 5, 7)
POS = tuple(ORDER.index(k) for k in range(8))


def _lanes(row):
    return jnp.transpose(jnp.broadcast_to(row, (128, 128)))


def _main(hid_hbm, wg_hbm, wu_hbm, wd_hbm, gain_hbm, wv_hbm, temp_hbm, tgt_hbm,
          out, small,
          w, wv, hid, act, yf, yall, ysend, yrecv, psend, precv0, precv, xbuf, kept, statm, stats, offs, invt, tgtm, gain, temp, tgt,
          in_sem, wf_sem, wd_sem, wv_sem,
          d2d_s, d2d_r, rs_s, rs_r, x_s, xa_r, xf_r, st_s, st_r, bulk_s, rxy, rd, rdl, pr, prd, prdl):
    me = lax.axis_index("tp")
    core = me % 2
    nx, ny, nd, pt = me ^ 2, me ^ 4, me ^ 6, me ^ 1

    def remote(src, dst, ss, rs, dev):
        return pltpu.make_async_remote_copy(src, dst, ss, rs, device_id={"tp": dev})

    def load(src, dst, sem):
        c = pltpu.make_async_copy(src, dst, sem)
        c.start()
        return c

    def load_wf(b):
        for t, ref in enumerate((wg_hbm, wu_hbm)):
            load(ref.at[:, pl.ds(b * FW, FW)], w.at[:, pl.ds(t * FL + b * FW, FW)], wf_sem.at[b])

    def wait_wf(b):
        both = w.at[:, pl.ds(0, 2 * FW)]
        pltpu.make_async_copy(wv_hbm.at[:, pl.ds(0, 2 * FW)], both, wf_sem.at[b]).wait()

    def load_wd(j):
        return load(wd_hbm.at[:, pl.ds(j * JW, JW)], w.at[pl.ds(j % 2 * FL, FL), pl.ds(2 * FL + j // 2 * JW, JW)], wd_sem.at[j])

    def load_wv(n):
        return load(wv_hbm.at[:, pl.ds(n * WW, WW)], wv.at[:, pl.ds(n * WW, WW)], wv_sem.at[n])

    hid_copy = load(hid_hbm, hid, in_sem.at[0])
    load_wf(0)
    small_copies = [load(temp_hbm, temp, in_sem.at[1]), load(tgt_hbm, tgt, in_sem.at[2]), load(gain_hbm, gain, in_sem.at[3])]
    for b in range(1, NF):
        load_wf(b)

    barrier = pltpu.get_barrier_semaphore()
    for k in range(1, 8):
        pl.semaphore_signal(barrier, inc=1, device_id={"tp": me ^ k})

    hid_copy.wait()
    wd_copies, wv_copies = [], []
    for b in range(NF):
        wait_wf(b)
        for j in range(b * NJ // NF, (b + 1) * NJ // NF):
            wd_copies.append(load_wd(j))
        if b == NF - 1:
            wv_copies.append(load_wv(0))
        g = jnp.dot(hid[...], w[:, b * FW:(b + 1) * FW], preferred_element_type=F32)
        u = jnp.dot(hid[...], w[:, FL + b * FW:FL + (b + 1) * FW], preferred_element_type=F32)
        act[:, b * FW:(b + 1) * FW] = (jax.nn.silu(g) * u).astype(BF16)

    def rows_of(dev):
        return pl.multiple_of((dev % 2) * HALF + (dev // 2) * PIECE, PIECE)

    keep = pl.multiple_of(core * HALF, HALF)
    give = pl.multiple_of(HALF - core * HALF, HALF)
    d2d = []
    for j in range(NJ):
        wd_copies[j].wait()
        if j < NW - 1:
            wv_copies.append(load_wv(j + 1))
        wd = w[j % 2 * FL:(j % 2 + 1) * FL, 2 * FL + j // 2 * JW:2 * FL + (j // 2 + 1) * JW]
        yf[:, j * JW:(j + 1) * JW] = jnp.dot(act[...], wd, preferred_element_type=F32)
        if j == 0:
            yall[...] = yf[:, 0:JW].astype(BF16)
            pl.semaphore_wait(barrier, 7)
            for k in (6, 7, 2, 3, 4, 5, 1):
                remote(yall.at[pl.ds(rows_of(me ^ k), PIECE), :], precv0.at[pl.ds((k - 1) * PIECE, PIECE), :],
                       rs_s, rs_r, me ^ k).start()
            continue
        ysend[:, (j - 1) * JW:j * JW] = yf[pl.ds(give, HALF), j * JW:(j + 1) * JW].astype(BF16)
        cols = pl.ds((j - 1) * JW, JW)
        c = remote(ysend.at[:, cols], yrecv.at[:, cols], d2d_s, d2d_r.at[j - 1], pt)
        c.start()
        d2d.append(c)

    for n in range(min(NJ + 1, NW), NW):
        wv_copies.append(load_wv(n))
    for c in small_copies:
        c.wait()
    offs[...] = _lanes(1.0 / temp[...])
    statm[...] = _lanes(tgt[...].astype(F32))
    for p, k in enumerate(ORDER):
        rows = pl.ds(rows_of(me ^ k), PIECE)
        invt[p * PIECE:(p + 1) * PIECE, :] = offs[rows, :]
        tgtm[p * PIECE:(p + 1) * PIECE, :] = statm[rows, :].astype(jnp.int32)

    def piece(dev):
        return pl.multiple_of((dev // 2) * PIECE, PIECE)

    for j in range(1, NJ):
        cols = slice(j * JW, (j + 1) * JW)
        d2d[j - 1].wait_recv()
        part = yf[pl.ds(keep, HALF), cols] + yrecv[:, (j - 1) * JW:j * JW].astype(F32)
        yf[pl.ds(keep, HALF), cols] = part
        psend[:, (j - 1) * JW:j * JW] = part.astype(BF16)
        if j in RS_ENDS:
            start = max([0] + [e for e in RS_ENDS if e < j])
            got = pl.ds(start * JW, (j - start) * JW)
            for s, dev in enumerate((nd, nx, ny)):
                remote(psend.at[pl.ds(piece(dev), PIECE), got], precv.at[pl.ds(s * PIECE, PIECE), got], rs_s, rs_r, dev).start()

    bytes_in = hid.at[pl.ds(0, (7 * JW + 3 * (D - JW)) * PIECE // D), :]
    rs_all = remote(bytes_in, bytes_in, rs_s, rs_r, nx)
    rs_all.wait_recv()
    mine = rows_of(me)
    y0 = yf[pl.ds(mine, PIECE), 0:JW]
    for k in range(7):
        y0 = y0 + precv0[k * PIECE:(k + 1) * PIECE, :].astype(F32)
    y1 = yf[pl.ds(mine, PIECE), JW:D]
    for s in range(3):
        y1 = y1 + precv[s * PIECE:(s + 1) * PIECE, :].astype(F32)
    y = jnp.concatenate([y0, y1], axis=-1)
    res = hid[pl.ds(mine, PIECE), :].astype(F32) + y
    inv_rms = lax.rsqrt(jnp.mean(res * res, axis=-1, keepdims=True) + NORM_EPS)
    xbuf[0:PIECE, :] = (gain[...] * res * inv_rms).astype(BF16)

    def xrow(k):
        return xbuf.at[pl.ds(POS[k] * PIECE, PIECE), :]

    for s, k in enumerate((6, 2, 4)):
        remote(xrow(0), xrow(k), x_s, xa_r.at[s], me ^ k).start()
    remote(xrow(0), xrow(1), x_s, xf_r, pt).start()

    def place(dev, i):
        row = pl.multiple_of((dev * 2 + i // GRID) * 128, 128)
        col = pl.multiple_of((i % GRID) * CW, CW)
        return row, pl.ds(col, CW)

    def block(dev, i, first, count, chunks=1):
        row, _ = place(dev, i)
        col = pl.multiple_of((i % GRID) * CW, CW)
        return w.at[pl.ds(row + first, count), pl.ds(col, chunks * CW)]

    def own_start(i, first, count, chunks=1):
        ref = block(me, i, first, count, chunks)
        remote(ref, ref, bulk_s, rxy.at[i // 2], nx).start()
        remote(ref, ref, bulk_s, rxy.at[i // 2], ny).start()
        remote(ref, ref, bulk_s, pr.at[i // 2], pt).start()

    def logits(i, first, count):
        acc = jnp.dot(xbuf[first:first + count, :], wv[:, pl.ds(pl.multiple_of(i * CW, CW), CW)], preferred_element_type=F32)
        scale = invt[first:first + count, :]
        return [acc[:, q * 128:(q + 1) * 128] * scale for q in range(CW // 128)]

    def row_max(parts):
        top = parts[0]
        for p in parts[1:]:
            top = jnp.maximum(top, p)
        return jnp.max(top, axis=-1, keepdims=True)

    def put(i, first, count, parts, top):
        row, _ = place(me, i)
        for q, p in enumerate(parts):
            w[pl.ds(row + first, count), pl.ds(pl.multiple_of((i % GRID) * CW + q * 128, 128), 128)] = (p - top).astype(BF16)

    def statistics(i, first, count, parts, top):
        total = weighted = hit = jnp.zeros((count, 128), F32)
        lane = lax.broadcasted_iota(jnp.int32, (count, 128), 1)
        ids = tgtm[first:first + count, :] - (me * VL + i * CW)
        for q, p in enumerate(parts):
            e = jnp.exp(p - top)
            total = total + e
            weighted = weighted + e * p
            hit = hit + jnp.where(ids == lane + q * 128, p, 0.0)
        sm = statm[first:first + count, :]
        sm = jnp.where(lane == i, top, sm)
        sm = jnp.where(lane == 16 + i, jnp.sum(total, axis=-1, keepdims=True), sm)
        sm = jnp.where(lane == 32 + i, jnp.sum(weighted, axis=-1, keepdims=True), sm)
        sm = jnp.where(lane == 48 + i, jnp.sum(hit, axis=-1, keepdims=True), sm)
        statm[first:first + count, :] = sm

    def head(i, first, count, go=False):
        parts = logits(i, first, count)
        top = row_max(parts)
        put(i, first, count, parts, top)
        if go:
            own_start(i, first, count)
        elif first:
            @pl.when(i < EARLY)
            def _():
                own_start(i, first, count)

        statistics(i, first, count, parts, top)

    def head_rest(i, _):
        head(i, PIECE, B - PIECE)
        return 0

    def head_all(i, _):
        head(i, 0, B)
        return 0

    def own_statistics(i, _):
        parts = [kept[:, pl.ds(pl.multiple_of(i * CW + q * 128, 128), 128)] for q in range(CW // 128)]
        statistics(i, 0, PIECE, parts, row_max(parts))
        return 0

    ready = 0
    for start in range(0, OWN, GROUP):
        group = range(start, min(start + GROUP, OWN))
        while ready * WW < (group[-1] + 1) * CW:
            wv_copies[ready].wait()
            ready += 1
        for i, parts in [(i, logits(i, 0, PIECE)) for i in group]:
            put(i, 0, PIECE, parts, row_max(parts))
            for q, p in enumerate(parts):
                kept[:, i * CW + q * 128:i * CW + (q + 1) * 128] = p
        own_start(start, 0, PIECE, len(group))
    for s, k in ((1, 2), (2, 4), (0, 6)):
        remote(xrow(k), xrow(k), x_s, xa_r.at[s], me ^ k).wait_recv()
        remote(xrow(k), xrow(k + 1), x_s, xf_r, pt).start()
    head(0, PIECE, HALF - PIECE, True)
    four = xbuf.at[pl.ds(0, 4 * PIECE), :]
    remote(four, four, x_s, xf_r, pt).wait_recv()
    head(0, HALF, HALF, True)
    for c in wv_copies[ready:]:
        c.wait()
    lax.fori_loop(1, OWN, head_rest, 0)
    lax.fori_loop(OWN, NC, head_all, 0)
    lax.fori_loop(0, OWN, own_statistics, 0)

    for p, k in enumerate(ORDER):
        offs[pl.ds(rows_of(me ^ k), PIECE), :] = statm[p * PIECE:(p + 1) * PIECE, :]
    st = jnp.transpose(offs[...])
    tops = st[0:NC, :]
    top = jnp.max(tops, axis=0, keepdims=True)
    scale = jnp.exp(tops - top)
    my_stats = jnp.concatenate(
        [tops, top, jnp.sum(scale * st[16:16 + NC, :], axis=0, keepdims=True),
         jnp.sum(scale * st[32:32 + NC, :], axis=0, keepdims=True),
         jnp.sum(st[48:48 + NC, :], axis=0, keepdims=True),
         jnp.zeros((16 - NC - 4, 128), F32)], axis=0)

    stats[0:16, :] = my_stats
    for k in range(1, 8):
        remote(stats.at[pl.ds(0, 16), :], stats.at[pl.ds(16 * k, 16), :], st_s, st_r, me ^ k).start()

    for i in range(EARLY, NC, 2):
        if i + 1 < OWN:
            own_start(i, PIECE, B - PIECE, 2)
        else:
            for n in (i, i + 1):
                own_start(n, PIECE if n < OWN else 0, B - PIECE if n < OWN else B)

    others = stats.at[pl.ds(16, 112), :]
    st_all = remote(others, others, st_s, st_r, nx)
    st_all.wait_recv()
    allst = [stats[16 * k:16 * (k + 1), :] for k in range(8)]
    top = allst[0][NC:NC + 1, :]
    for s in allst[1:]:
        top = jnp.maximum(top, s[NC:NC + 1, :])
    total = weighted = hit = jnp.zeros((1, 128), F32)
    for s in allst:
        scale = jnp.exp(s[NC:NC + 1, :] - top)
        total = total + scale * s[NC + 1:NC + 2, :]
        weighted = weighted + scale * s[NC + 2:NC + 3, :]
        hit = hit + s[NC + 3:NC + 4, :]
    log_norm = top + jnp.log(total)
    small[0:1, :] = log_norm
    small[1:2, :] = log_norm - weighted / total
    small[2:3, :] = hit - log_norm
    small[3:8, :] = jnp.zeros((5, 128), F32)
    offs[...] = jnp.transpose(stats[...] - log_norm)

    lane16 = lax.broadcasted_iota(jnp.int32, (PIECE, 128), 1)

    def fix(rel, i, first=0, count=8):
        dev = me ^ rel
        row, cols = place(dev, i)
        for k in range(first, first + count):
            rows = pl.ds(rows_of(dev ^ ORDER[k]), PIECE)
            off = jnp.sum(jnp.where(lane16 == rel * 16 + i, offs[rows, :], 0.0), axis=-1, keepdims=True)
            val = w[pl.ds(row + k * PIECE, PIECE), cols].astype(F32) + off
            out[rows, pl.ds(pl.multiple_of(dev * VL + i * CW, CW), CW)] = val.astype(BF16)

    def arrived(n, sem):
        ref = w.at[pl.ds(0, n * PIECE), pl.ds(0, CW)]
        remote(ref, ref, bulk_s, sem, nx).wait_recv()

    def send(ref, sem, to):
        remote(ref, ref, bulk_s, sem, to).start()

    def both(rel, p):
        fix(rel, 2 * p)
        fix(rel, 2 * p + 1)

    def arrivals(p, _):
        arrived(32, rxy.at[p])
        if isinstance(p, int):
            for n in range(NS):
                first, count = CUTS[n] * PIECE, (CUTS[n + 1] - CUTS[n]) * PIECE
                for rel, i, to in ((2, 2 * p, ny), (4, 2 * p + 1, nx)):
                    ref = block(me ^ rel, i, first, count)
                    send(ref, rdl.at[n], to)
                    if n == NS - 1:
                        send(ref, prdl.at[n], to ^ 1)
        else:
            send(block(nx, 2 * p, 0, B), rd.at[p], ny)
            send(block(ny, 2 * p + 1, 0, B), rd.at[p], nx)
        send(block(nx, 2 * p, 0, B, 2), pr.at[p], pt)
        send(block(ny, 2 * p, 0, B, 2), pr.at[p], pt)
        both(0, p)
        both(2, p)
        both(4, p)
        arrived(48, pr.at[p])
        both(1, p)
        both(3, p)
        both(5, p)
        return 0

    lax.fori_loop(0, NP - 1, arrivals, 0)
    arrivals(NP - 1, 0)

    for p in range(NP - 1):
        arrived(16, rd.at[p])
        send(block(nd, 2 * p, 0, B, 2), prd.at[p], pt)
        both(6, p)
        if p:
            arrived(16, prd.at[p - 1])
            both(7, p - 1)
    for n in range(NS):
        count = CUTS[n + 1] - CUTS[n]
        arrived(2 * count, rdl.at[n])
        if n < NS - 1:
            send(block(nd, NC - 2, CUTS[n] * PIECE, count * PIECE, 2), prdl.at[n], pt)
        for i in (NC - 2, NC - 1):
            fix(6, i, CUTS[n], count)
        if n == 0:
            arrived(16, prd.at[NP - 2])
            both(7, NP - 2)
    for n in range(NS):
        count = CUTS[n + 1] - CUTS[n]
        arrived(2 * count, prdl.at[n])
        for i in (NC - 2, NC - 1):
            fix(7, i, CUTS[n], count)

    def left(ref, sem):
        remote(ref, ref, sem, rs_r, nx).wait_send()

    left(ysend, d2d_s)
    rs_all.wait_send()
    left(xbuf.at[pl.ds(0, 7 * PIECE), :], x_s)
    st_all.wait_send()
    left(w.at[pl.ds(0, 1792), :], bulk_s)


def _write(src, small, out, o0, o1, o2, sem):
    step = B // 16
    cs = [pltpu.make_async_copy(small.at[pl.ds(k, 1), :], o, sem.at[k]) for k, o in enumerate((o0, o1, o2))]
    for k in range(16):
        pltpu.make_async_copy(src.at[pl.ds(k * step, step)], out.at[pl.ds(k * step, step)], sem.at[3]).start()
    for c in cs:
        c.start()
    for c in cs:
        c.wait()
    pltpu.make_async_copy(src, out, sem.at[3]).wait()


def solution(mesh):
    vmem = pl.BlockSpec(memory_space=pltpu.VMEM)
    hbm = pl.BlockSpec(memory_space=pltpu.HBM)
    dma = pltpu.SemaphoreType.DMA

    def device_step(hidden, w_gate, w_up, w_down, norm_gain, w_vocab, temperature, target):
        wide, small = pl.pallas_call(
            _main,
            out_shape=(pltpu.VMEM((B, V), BF16), pltpu.VMEM((8, 128), F32)),
            in_specs=[hbm] * 8,
            out_specs=(vmem, vmem),
            scratch_shapes=[
                pltpu.VMEM((2048, 3072), BF16), pltpu.VMEM((D, VL), BF16), pltpu.VMEM((B, D), BF16),
                pltpu.VMEM((B, FL), BF16), pltpu.VMEM((B, D), F32), pltpu.VMEM((B, JW), BF16), pltpu.VMEM((HALF, D - JW), BF16),
                pltpu.VMEM((HALF, D - JW), BF16), pltpu.VMEM((HALF, D - JW), BF16), pltpu.VMEM((7 * PIECE, JW), BF16),
                pltpu.VMEM((3 * PIECE, D - JW), BF16),
                pltpu.VMEM((B, D), BF16), pltpu.VMEM((PIECE, OWN * CW), F32), pltpu.VMEM((128, 128), F32), pltpu.VMEM((128, 128), F32),
                pltpu.VMEM((128, 128), F32), pltpu.VMEM((128, 128), F32), pltpu.VMEM((128, 128), jnp.int32),
                pltpu.VMEM((1, D), F32), pltpu.VMEM((1, B), F32), pltpu.VMEM((1, B), jnp.int32),
                dma((4,)), dma((NF,)), dma((NJ,)), dma((NW,)),
                dma, dma((NJ - 1,)), dma, dma, dma, dma((3,)), dma, dma, dma, dma,
                dma((NP,)), dma((NP - 1,)), dma((NS,)), dma((NP,)), dma((NP - 1,)), dma((NS,)),
            ],
            compiler_params=pltpu.CompilerParams(collective_id=0, has_side_effects=True, vmem_limit_bytes=49 << 20),
            name="step",
        )(hidden, w_gate, w_up, w_down, norm_gain.reshape(1, D), w_vocab, temperature.reshape(1, B), target.reshape(1, B))
        row = jax.ShapeDtypeStruct((1, B), F32)
        log_probs, log_norm, entropy, target_logp = pl.pallas_call(
            _write,
            out_shape=(jax.ShapeDtypeStruct((B, V), BF16), row, row, row),
            in_specs=[vmem, vmem],
            out_specs=(hbm, hbm, hbm, hbm),
            scratch_shapes=[dma((4,))],
            compiler_params=pltpu.CompilerParams(vmem_limit_bytes=16 << 20),
            name="write",
        )(wide, small)
        return log_norm.reshape(B), entropy.reshape(B), target_logp.reshape(B), log_probs

    return jax.shard_map(
        device_step,
        mesh=mesh,
        in_specs=(P("dp", None), P(None, "tp"), P(None, "tp"), P("tp", None), P(None),
                  P(None, "tp"), P("dp"), P("dp")),
        out_specs=(P("dp"), P("dp"), P("dp"), P("dp", None)),
        check_vma=False,
    )
```

```python
import jax
import jax.numpy as jnp
from jax import lax
from jax.experimental import pallas as pl
from jax.experimental.pallas import tpu as pltpu
from jax.sharding import PartitionSpec as P

NORM_EPS = 1e-6
F32 = jnp.float32
BF16 = jnp.bfloat16
B, D, FL, V, VL = 128, 2048, 1024, 49152, 6144
NC = 8
CW = VL // NC
GRID = 3072 // CW
EARLY = 4
OWN = 7
GROUP = 2
NP = NC // 2
CUTS = (0, 5, 7, 8)
NS = len(CUTS) - 1
FCUTS = (0, 256, 768, 1024)
NF = len(FCUTS) - 1
WD_AT = (1, 2, 4)
NJ = 4
JW = D // NJ
RS_ENDS = (1, 2, 3)
HALF, PIECE = 64, 16
NW = 4
WW = VL // NW


ORDER = (0, 2, 4, 6, 1, 3, 5, 7)
POS = tuple(ORDER.index(k) for k in range(8))


def _lanes(row):
    return jnp.transpose(jnp.broadcast_to(row, (128, 128)))


def _main(hid_hbm, wg_hbm, wu_hbm, wd_hbm, gain_hbm, wv_hbm, temp_hbm, tgt_hbm,
          out, small,
          w, wv, hid, act, yf, yall, ysend, yrecv, psend, precv0, precv, xbuf, kept, statm, stats, offs, invt, tgtm, gain, temp, tgt,
          in_sem, wf_sem, wd_sem, wv_sem,
          d2d_s, d2d_r, rs_s, rs_r, x_s, xa_r, xf_r, st_s, st_r, bulk_s, rxy, rd, rdl, pr, prd, prdl):
    me = lax.axis_index("tp")
    core = me % 2
    nx, ny, nd, pt = me ^ 2, me ^ 4, me ^ 6, me ^ 1

    def remote(src, dst, ss, rs, dev):
        return pltpu.make_async_remote_copy(src, dst, ss, rs, device_id={"tp": dev})

    def load(src, dst, sem):
        c = pltpu.make_async_copy(src, dst, sem)
        c.start()
        return c

    def load_wf(b):
        for t, ref in enumerate((wg_hbm, wu_hbm)):
            start, width = FCUTS[b], FCUTS[b + 1] - FCUTS[b]
            load(ref.at[:, pl.ds(start, width)], w.at[:, pl.ds(t * FL + start, width)], wf_sem.at[b])

    def wait_wf(b):
        width = 2 * (FCUTS[b + 1] - FCUTS[b])
        pltpu.make_async_copy(wv_hbm.at[:, pl.ds(0, width)], w.at[:, pl.ds(0, width)], wf_sem.at[b]).wait()

    def load_wd(j):
        return load(wd_hbm.at[:, pl.ds(j * JW, JW)], w.at[pl.ds(j % 2 * FL, FL), pl.ds(2 * FL + j // 2 * JW, JW)], wd_sem.at[j])

    def load_wv(n):
        return load(wv_hbm.at[:, pl.ds(n * WW, WW)], wv.at[:, pl.ds(n * WW, WW)], wv_sem.at[n])

    hid_copy = load(hid_hbm, hid, in_sem.at[0])
    load_wf(0)
    small_copies = [load(temp_hbm, temp, in_sem.at[1]), load(tgt_hbm, tgt, in_sem.at[2]), load(gain_hbm, gain, in_sem.at[3])]
    for b in range(1, NF):
        load_wf(b)

    barrier = pltpu.get_barrier_semaphore()
    for k in range(1, 8):
        pl.semaphore_signal(barrier, inc=1, device_id={"tp": me ^ k})

    hid_copy.wait()
    wd_copies, wv_copies = [], []
    for b in range(NF):
        wait_wf(b)
        for j in range(len(wd_copies), WD_AT[b]):
            wd_copies.append(load_wd(j))
        g = jnp.dot(hid[...], w[:, FCUTS[b]:FCUTS[b + 1]], preferred_element_type=F32)
        u = jnp.dot(hid[...], w[:, FL + FCUTS[b]:FL + FCUTS[b + 1]], preferred_element_type=F32)
        act[:, FCUTS[b]:FCUTS[b + 1]] = (jax.nn.silu(g) * u).astype(BF16)

    def rows_of(dev):
        return pl.multiple_of((dev % 2) * HALF + (dev // 2) * PIECE, PIECE)

    keep = pl.multiple_of(core * HALF, HALF)
    give = pl.multiple_of(HALF - core * HALF, HALF)
    d2d = []
    for j in range(NJ):
        wd_copies[j].wait()
        if j < NW:
            wv_copies.append(load_wv(j))
        wd = w[j % 2 * FL:(j % 2 + 1) * FL, 2 * FL + j // 2 * JW:2 * FL + (j // 2 + 1) * JW]
        yf[:, j * JW:(j + 1) * JW] = jnp.dot(act[...], wd, preferred_element_type=F32)
        if j == 0:
            yall[...] = yf[:, 0:JW].astype(BF16)
            pl.semaphore_wait(barrier, 7)
            for k in (6, 7, 2, 3, 4, 5, 1):
                remote(yall.at[pl.ds(rows_of(me ^ k), PIECE), :], precv0.at[pl.ds((k - 1) * PIECE, PIECE), :],
                       rs_s, rs_r, me ^ k).start()
            continue
        ysend[:, (j - 1) * JW:j * JW] = yf[pl.ds(give, HALF), j * JW:(j + 1) * JW].astype(BF16)
        cols = pl.ds((j - 1) * JW, JW)
        c = remote(ysend.at[:, cols], yrecv.at[:, cols], d2d_s, d2d_r.at[j - 1], pt)
        c.start()
        d2d.append(c)

    for n in range(min(NJ, NW), NW):
        wv_copies.append(load_wv(n))
    for c in small_copies:
        c.wait()
    offs[...] = _lanes(1.0 / temp[...])
    statm[...] = _lanes(tgt[...].astype(F32))
    for p, k in enumerate(ORDER):
        rows = pl.ds(rows_of(me ^ k), PIECE)
        invt[p * PIECE:(p + 1) * PIECE, :] = offs[rows, :]
        tgtm[p * PIECE:(p + 1) * PIECE, :] = statm[rows, :].astype(jnp.int32)

    def piece(dev):
        return pl.multiple_of((dev // 2) * PIECE, PIECE)

    for j in range(1, NJ):
        cols = slice(j * JW, (j + 1) * JW)
        d2d[j - 1].wait_recv()
        part = yf[pl.ds(keep, HALF), cols] + yrecv[:, (j - 1) * JW:j * JW].astype(F32)
        yf[pl.ds(keep, HALF), cols] = part
        psend[:, (j - 1) * JW:j * JW] = part.astype(BF16)
        if j in RS_ENDS:
            start = max([0] + [e for e in RS_ENDS if e < j])
            got = pl.ds(start * JW, (j - start) * JW)
            for s, dev in enumerate((nd, nx, ny)):
                remote(psend.at[pl.ds(piece(dev), PIECE), got], precv.at[pl.ds(s * PIECE, PIECE), got], rs_s, rs_r, dev).start()

    bytes_in = hid.at[pl.ds(0, (7 * JW + 3 * (D - JW)) * PIECE // D), :]
    rs_all = remote(bytes_in, bytes_in, rs_s, rs_r, nx)
    rs_all.wait_recv()
    mine = rows_of(me)
    y0 = yf[pl.ds(mine, PIECE), 0:JW]
    for k in range(7):
        y0 = y0 + precv0[k * PIECE:(k + 1) * PIECE, :].astype(F32)
    y1 = yf[pl.ds(mine, PIECE), JW:D]
    for s in range(3):
        y1 = y1 + precv[s * PIECE:(s + 1) * PIECE, :].astype(F32)
    y = jnp.concatenate([y0, y1], axis=-1)
    res = hid[pl.ds(mine, PIECE), :].astype(F32) + y
    inv_rms = lax.rsqrt(jnp.mean(res * res, axis=-1, keepdims=True) + NORM_EPS)
    xbuf[0:PIECE, :] = (gain[...] * res * inv_rms).astype(BF16)

    def xrow(k):
        return xbuf.at[pl.ds(POS[k] * PIECE, PIECE), :]

    for s, k in enumerate((6, 2, 4)):
        remote(xrow(0), xrow(k), x_s, xa_r.at[s], me ^ k).start()
    remote(xrow(0), xrow(1), x_s, xf_r, pt).start()

    def place(dev, i):
        row = pl.multiple_of((dev * 2 + i // GRID) * 128, 128)
        col = pl.multiple_of((i % GRID) * CW, CW)
        return row, pl.ds(col, CW)

    def block(dev, i, first, count, chunks=1):
        row, _ = place(dev, i)
        col = pl.multiple_of((i % GRID) * CW, CW)
        return w.at[pl.ds(row + first, count), pl.ds(col, chunks * CW)]

    def own_start(i, first, count, chunks=1):
        ref = block(me, i, first, count, chunks)
        remote(ref, ref, bulk_s, rxy.at[i // 2], nx).start()
        remote(ref, ref, bulk_s, rxy.at[i // 2], ny).start()
        remote(ref, ref, bulk_s, pr.at[i // 2], pt).start()

    def logits(i, first, count):
        acc = jnp.dot(xbuf[first:first + count, :], wv[:, pl.ds(pl.multiple_of(i * CW, CW), CW)], preferred_element_type=F32)
        scale = invt[first:first + count, :]
        return [acc[:, q * 128:(q + 1) * 128] * scale for q in range(CW // 128)]

    def row_max(parts):
        top = parts[0]
        for p in parts[1:]:
            top = jnp.maximum(top, p)
        return jnp.max(top, axis=-1, keepdims=True)

    def put(i, first, count, parts, top):
        row, _ = place(me, i)
        for q, p in enumerate(parts):
            w[pl.ds(row + first, count), pl.ds(pl.multiple_of((i % GRID) * CW + q * 128, 128), 128)] = (p - top).astype(BF16)

    def statistics(i, first, count, parts, top):
        total = weighted = hit = jnp.zeros((count, 128), F32)
        lane = lax.broadcasted_iota(jnp.int32, (count, 128), 1)
        ids = tgtm[first:first + count, :] - (me * VL + i * CW)
        for q, p in enumerate(parts):
            e = jnp.exp(p - top)
            total = total + e
            weighted = weighted + e * p
            hit = hit + jnp.where(ids == lane + q * 128, p, 0.0)
        sm = statm[first:first + count, :]
        sm = jnp.where(lane == i, top, sm)
        sm = jnp.where(lane == 16 + i, jnp.sum(total, axis=-1, keepdims=True), sm)
        sm = jnp.where(lane == 32 + i, jnp.sum(weighted, axis=-1, keepdims=True), sm)
        sm = jnp.where(lane == 48 + i, jnp.sum(hit, axis=-1, keepdims=True), sm)
        statm[first:first + count, :] = sm

    def head(i, first, count, go=False):
        parts = logits(i, first, count)
        top = row_max(parts)
        put(i, first, count, parts, top)
        if go:
            own_start(i, first, count)
        elif first:
            @pl.when(i < EARLY)
            def _():
                own_start(i, first, count)

        statistics(i, first, count, parts, top)

    def head_rest(i, _):
        head(i, PIECE, B - PIECE)
        return 0

    def head_all(i, _):
        head(i, 0, B)
        return 0

    def own_statistics(i, _):
        parts = [kept[:, pl.ds(pl.multiple_of(i * CW + q * 128, 128), 128)] for q in range(CW // 128)]
        statistics(i, 0, PIECE, parts, row_max(parts))
        return 0

    ready = 0
    for start in range(0, OWN, GROUP):
        group = range(start, min(start + GROUP, OWN))
        while ready * WW < (group[-1] + 1) * CW:
            wv_copies[ready].wait()
            ready += 1
        for i, parts in [(i, logits(i, 0, PIECE)) for i in group]:
            put(i, 0, PIECE, parts, row_max(parts))
            for q, p in enumerate(parts):
                kept[:, i * CW + q * 128:i * CW + (q + 1) * 128] = p
        own_start(start, 0, PIECE, len(group))
    for s, k in ((1, 2), (2, 4), (0, 6)):
        remote(xrow(k), xrow(k), x_s, xa_r.at[s], me ^ k).wait_recv()
        remote(xrow(k), xrow(k + 1), x_s, xf_r, pt).start()
    head(0, PIECE, HALF - PIECE, True)
    four = xbuf.at[pl.ds(0, 4 * PIECE), :]
    remote(four, four, x_s, xf_r, pt).wait_recv()
    head(0, HALF, HALF, True)
    for c in wv_copies[ready:]:
        c.wait()
    lax.fori_loop(1, OWN, head_rest, 0)
    lax.fori_loop(OWN, NC, head_all, 0)
    lax.fori_loop(0, OWN, own_statistics, 0)

    for p, k in enumerate(ORDER):
        offs[pl.ds(rows_of(me ^ k), PIECE), :] = statm[p * PIECE:(p + 1) * PIECE, :]
    st = jnp.transpose(offs[...])
    tops = st[0:NC, :]
    top = jnp.max(tops, axis=0, keepdims=True)
    scale = jnp.exp(tops - top)
    my_stats = jnp.concatenate(
        [tops, top, jnp.sum(scale * st[16:16 + NC, :], axis=0, keepdims=True),
         jnp.sum(scale * st[32:32 + NC, :], axis=0, keepdims=True),
         jnp.sum(st[48:48 + NC, :], axis=0, keepdims=True),
         jnp.zeros((16 - NC - 4, 128), F32)], axis=0)

    stats[0:16, :] = my_stats
    for k in range(1, 8):
        remote(stats.at[pl.ds(0, 16), :], stats.at[pl.ds(16 * k, 16), :], st_s, st_r, me ^ k).start()

    for i in range(EARLY, NC, 2):
        if i + 1 < OWN:
            own_start(i, PIECE, B - PIECE, 2)
        else:
            for n in (i, i + 1):
                own_start(n, PIECE if n < OWN else 0, B - PIECE if n < OWN else B)

    others = stats.at[pl.ds(16, 112), :]
    st_all = remote(others, others, st_s, st_r, nx)
    st_all.wait_recv()
    allst = [stats[16 * k:16 * (k + 1), :] for k in range(8)]
    top = allst[0][NC:NC + 1, :]
    for s in allst[1:]:
        top = jnp.maximum(top, s[NC:NC + 1, :])
    total = weighted = hit = jnp.zeros((1, 128), F32)
    for s in allst:
        scale = jnp.exp(s[NC:NC + 1, :] - top)
        total = total + scale * s[NC + 1:NC + 2, :]
        weighted = weighted + scale * s[NC + 2:NC + 3, :]
        hit = hit + s[NC + 3:NC + 4, :]
    log_norm = top + jnp.log(total)
    small[0:1, :] = log_norm
    small[1:2, :] = log_norm - weighted / total
    small[2:3, :] = hit - log_norm
    small[3:8, :] = jnp.zeros((5, 128), F32)
    offs[...] = jnp.transpose(stats[...] - log_norm)

    lane16 = lax.broadcasted_iota(jnp.int32, (PIECE, 128), 1)

    def fix(rel, i, first=0, count=8):
        dev = me ^ rel
        row, cols = place(dev, i)
        for k in range(first, first + count):
            rows = pl.ds(rows_of(dev ^ ORDER[k]), PIECE)
            off = jnp.sum(jnp.where(lane16 == rel * 16 + i, offs[rows, :], 0.0), axis=-1, keepdims=True)
            val = w[pl.ds(row + k * PIECE, PIECE), cols].astype(F32) + off
            out[rows, pl.ds(pl.multiple_of(dev * VL + i * CW, CW), CW)] = val.astype(BF16)

    def arrived(n, sem):
        ref = w.at[pl.ds(0, n * PIECE), pl.ds(0, CW)]
        remote(ref, ref, bulk_s, sem, nx).wait_recv()

    def send(ref, sem, to):
        remote(ref, ref, bulk_s, sem, to).start()

    def both(rel, p):
        fix(rel, 2 * p)
        fix(rel, 2 * p + 1)

    def arrivals(p, _):
        arrived(32, rxy.at[p])
        if isinstance(p, int):
            for n in range(NS):
                first, count = CUTS[n] * PIECE, (CUTS[n + 1] - CUTS[n]) * PIECE
                for rel, i, to in ((2, 2 * p, ny), (4, 2 * p + 1, nx)):
                    ref = block(me ^ rel, i, first, count)
                    send(ref, rdl.at[n], to)
                    if n == NS - 1:
                        send(ref, prdl.at[n], to ^ 1)
        else:
            send(block(nx, 2 * p, 0, B), rd.at[p], ny)
            send(block(ny, 2 * p + 1, 0, B), rd.at[p], nx)
        send(block(nx, 2 * p, 0, B, 2), pr.at[p], pt)
        send(block(ny, 2 * p, 0, B, 2), pr.at[p], pt)
        both(0, p)
        both(2, p)
        both(4, p)
        arrived(48, pr.at[p])
        both(1, p)
        both(3, p)
        both(5, p)
        return 0

    lax.fori_loop(0, NP - 1, arrivals, 0)
    arrivals(NP - 1, 0)

    for p in range(NP - 1):
        arrived(16, rd.at[p])
        send(block(nd, 2 * p, 0, B, 2), prd.at[p], pt)
        both(6, p)
        if p:
            arrived(16, prd.at[p - 1])
            both(7, p - 1)
    for n in range(NS):
        count = CUTS[n + 1] - CUTS[n]
        arrived(2 * count, rdl.at[n])
        if n < NS - 1:
            send(block(nd, NC - 2, CUTS[n] * PIECE, count * PIECE, 2), prdl.at[n], pt)
        for i in (NC - 2, NC - 1):
            fix(6, i, CUTS[n], count)
        if n == 0:
            arrived(16, prd.at[NP - 2])
            both(7, NP - 2)
    for n in range(NS):
        count = CUTS[n + 1] - CUTS[n]
        arrived(2 * count, prdl.at[n])
        for i in (NC - 2, NC - 1):
            fix(7, i, CUTS[n], count)

    def left(ref, sem):
        remote(ref, ref, sem, rs_r, nx).wait_send()

    left(ysend, d2d_s)
    rs_all.wait_send()
    left(xbuf.at[pl.ds(0, 7 * PIECE), :], x_s)
    st_all.wait_send()
    left(w.at[pl.ds(0, 1792), :], bulk_s)


def _write(src, small, out, o0, o1, o2, sem):
    step = B // 16
    cs = [pltpu.make_async_copy(small.at[pl.ds(k, 1), :], o, sem.at[k]) for k, o in enumerate((o0, o1, o2))]
    for k in range(16):
        for c in range(4):
            at = (pl.ds(k * step, step), pl.ds(c * (V // 4), V // 4))
            pltpu.make_async_copy(src.at[at], out.at[at], sem.at[3]).start()
    for c in cs:
        c.start()
    for c in cs:
        c.wait()
    pltpu.make_async_copy(src, out, sem.at[3]).wait()


def solution(mesh):
    vmem = pl.BlockSpec(memory_space=pltpu.VMEM)
    hbm = pl.BlockSpec(memory_space=pltpu.HBM)
    dma = pltpu.SemaphoreType.DMA

    def device_step(hidden, w_gate, w_up, w_down, norm_gain, w_vocab, temperature, target):
        wide, small = pl.pallas_call(
            _main,
            out_shape=(pltpu.VMEM((B, V), BF16), pltpu.VMEM((8, 128), F32)),
            in_specs=[hbm] * 8,
            out_specs=(vmem, vmem),
            scratch_shapes=[
                pltpu.VMEM((2048, 3072), BF16), pltpu.VMEM((D, VL), BF16), pltpu.VMEM((B, D), BF16),
                pltpu.VMEM((B, FL), BF16), pltpu.VMEM((B, D), F32), pltpu.VMEM((B, JW), BF16), pltpu.VMEM((HALF, D - JW), BF16),
                pltpu.VMEM((HALF, D - JW), BF16), pltpu.VMEM((HALF, D - JW), BF16), pltpu.VMEM((7 * PIECE, JW), BF16),
                pltpu.VMEM((3 * PIECE, D - JW), BF16),
                pltpu.VMEM((B, D), BF16), pltpu.VMEM((PIECE, OWN * CW), F32), pltpu.VMEM((128, 128), F32), pltpu.VMEM((128, 128), F32),
                pltpu.VMEM((128, 128), F32), pltpu.VMEM((128, 128), F32), pltpu.VMEM((128, 128), jnp.int32),
                pltpu.VMEM((1, D), F32), pltpu.VMEM((1, B), F32), pltpu.VMEM((1, B), jnp.int32),
                dma((4,)), dma((NF,)), dma((NJ,)), dma((NW,)),
                dma, dma((NJ - 1,)), dma, dma, dma, dma((3,)), dma, dma, dma, dma,
                dma((NP,)), dma((NP - 1,)), dma((NS,)), dma((NP,)), dma((NP - 1,)), dma((NS,)),
            ],
            compiler_params=pltpu.CompilerParams(collective_id=0, has_side_effects=True, vmem_limit_bytes=49 << 20),
            name="step",
        )(hidden, w_gate, w_up, w_down, norm_gain.reshape(1, D), w_vocab, temperature.reshape(1, B), target.reshape(1, B))
        row = jax.ShapeDtypeStruct((1, B), F32)
        log_probs, log_norm, entropy, target_logp = pl.pallas_call(
            _write,
            out_shape=(jax.ShapeDtypeStruct((B, V), BF16), row, row, row),
            in_specs=[vmem, vmem],
            out_specs=(hbm, hbm, hbm, hbm),
            scratch_shapes=[dma((4,))],
            compiler_params=pltpu.CompilerParams(vmem_limit_bytes=16 << 20),
            name="write",
        )(wide, small)
        return log_norm.reshape(B), entropy.reshape(B), target_logp.reshape(B), log_probs

    return jax.shard_map(
        device_step,
        mesh=mesh,
        in_specs=(P("dp", None), P(None, "tp"), P(None, "tp"), P("tp", None), P(None),
                  P(None, "tp"), P("dp"), P("dp")),
        out_specs=(P("dp"), P("dp"), P("dp"), P("dp", None)),
        check_vma=False,
    )
```

```python
import jax
import jax.numpy as jnp
from jax import lax
from jax.experimental import pallas as pl
from jax.experimental.pallas import tpu as pltpu
from jax.sharding import PartitionSpec as P

NORM_EPS = 1e-6
F32 = jnp.float32
BF16 = jnp.bfloat16
B, D, FL, V, VL = 128, 2048, 1024, 49152, 6144
NC = 8
CW = VL // NC
GRID = 3072 // CW
EARLY = 4
OWN = 7
GROUP = 2
NP = NC // 2
CUTS = (0, 6, 7, 8)
NS = len(CUTS) - 1
FCUTS = (0, 256, 768, 1024)
NF = len(FCUTS) - 1
WD_AT = (1, 2, 4)
NJ = 4
JW = D // NJ
HALF, PIECE = 64, 16
NW = 4
WW = VL // NW


ORDER = (0, 2, 4, 6, 1, 3, 5, 7)
POS = tuple(ORDER.index(k) for k in range(8))


def _lanes(row):
    return jnp.transpose(jnp.broadcast_to(row, (128, 128)))


def _main(hid_hbm, wg_hbm, wu_hbm, wd_hbm, gain_hbm, wv_hbm, temp_hbm, tgt_hbm,
          out, small,
          w, wv, hid, act, yf, yall, ysend, yrecv, psend, precv0, precv, xbuf, kept, statm, stats, offs, invt, tgtm, gain, temp, tgt,
          in_sem, wf_sem, wd_sem, wv_sem,
          d2d_s, d2d_r, rs_s, rs_r, x_s, xa_r, xf_r, st_s, st_r, bulk_s, rxy, rd, rdl, pr, prd, prdl):
    me = lax.axis_index("tp")
    core = me % 2
    nx, ny, nd, pt = me ^ 2, me ^ 4, me ^ 6, me ^ 1

    def remote(src, dst, ss, rs, dev):
        return pltpu.make_async_remote_copy(src, dst, ss, rs, device_id={"tp": dev})

    def load(src, dst, sem):
        c = pltpu.make_async_copy(src, dst, sem)
        c.start()
        return c

    def load_wf(b):
        for t, ref in enumerate((wg_hbm, wu_hbm)):
            start, width = FCUTS[b], FCUTS[b + 1] - FCUTS[b]
            load(ref.at[:, pl.ds(start, width)], w.at[:, pl.ds(t * FL + start, width)], wf_sem.at[b])

    def wait_wf(b):
        width = 2 * (FCUTS[b + 1] - FCUTS[b])
        pltpu.make_async_copy(wv_hbm.at[:, pl.ds(0, width)], w.at[:, pl.ds(0, width)], wf_sem.at[b]).wait()

    def load_wd(j):
        return load(wd_hbm.at[:, pl.ds(j * JW, JW)], w.at[pl.ds(j % 2 * FL, FL), pl.ds(2 * FL + j // 2 * JW, JW)], wd_sem.at[j])

    def load_wv(n):
        return load(wv_hbm.at[:, pl.ds(n * WW, WW)], wv.at[:, pl.ds(n * WW, WW)], wv_sem.at[n])

    hid_copy = load(hid_hbm, hid, in_sem.at[0])
    load_wf(0)
    small_copies = [load(temp_hbm, temp, in_sem.at[1]), load(tgt_hbm, tgt, in_sem.at[2]), load(gain_hbm, gain, in_sem.at[3])]
    for b in range(1, NF):
        load_wf(b)

    barrier = pltpu.get_barrier_semaphore()
    for k in range(1, 8):
        pl.semaphore_signal(barrier, inc=1, device_id={"tp": me ^ k})

    hid_copy.wait()
    wd_copies, wv_copies = [], []
    for b in range(NF):
        wait_wf(b)
        for j in range(len(wd_copies), WD_AT[b]):
            wd_copies.append(load_wd(j))
        g = jnp.dot(hid[...], w[:, FCUTS[b]:FCUTS[b + 1]], preferred_element_type=F32)
        u = jnp.dot(hid[...], w[:, FL + FCUTS[b]:FL + FCUTS[b + 1]], preferred_element_type=F32)
        act[:, FCUTS[b]:FCUTS[b + 1]] = (jax.nn.silu(g) * u).astype(BF16)

    def rows_of(dev):
        return pl.multiple_of((dev % 2) * HALF + (dev // 2) * PIECE, PIECE)

    keep = pl.multiple_of(core * HALF, HALF)
    give = pl.multiple_of(HALF - core * HALF, HALF)
    d2d = []
    for j in range(NJ):
        wd_copies[j].wait()
        if j < NW:
            wv_copies.append(load_wv(j))
        wd = w[j % 2 * FL:(j % 2 + 1) * FL, 2 * FL + j // 2 * JW:2 * FL + (j // 2 + 1) * JW]
        yf[:, j * JW:(j + 1) * JW] = jnp.dot(act[...], wd, preferred_element_type=F32)
        if j == 0:
            yall[...] = yf[:, 0:JW].astype(BF16)
            pl.semaphore_wait(barrier, 7)
            for k in (6, 7, 2, 3, 4, 5, 1):
                remote(yall.at[pl.ds(rows_of(me ^ k), PIECE), :], precv0.at[pl.ds((k - 1) * PIECE, PIECE), :],
                       rs_s, rs_r, me ^ k).start()
            continue
        rows = pl.ds((j - 1) * HALF, HALF)
        ysend[rows, :] = yf[pl.ds(give, HALF), j * JW:(j + 1) * JW].astype(BF16)
        c = remote(ysend.at[rows, :], yrecv.at[rows, :], d2d_s, d2d_r.at[j - 1], pt)
        c.start()
        d2d.append(c)

    for n in range(min(NJ, NW), NW):
        wv_copies.append(load_wv(n))
    for c in small_copies:
        c.wait()
    offs[...] = _lanes(1.0 / temp[...])
    statm[...] = _lanes(tgt[...].astype(F32))
    for p, k in enumerate(ORDER):
        rows = pl.ds(rows_of(me ^ k), PIECE)
        invt[p * PIECE:(p + 1) * PIECE, :] = offs[rows, :]
        tgtm[p * PIECE:(p + 1) * PIECE, :] = statm[rows, :].astype(jnp.int32)

    def piece(dev):
        return pl.multiple_of((dev // 2) * PIECE, PIECE)

    for j in range(1, NJ):
        cols = slice(j * JW, (j + 1) * JW)
        d2d[j - 1].wait_recv()
        part = yf[pl.ds(keep, HALF), cols] + yrecv[(j - 1) * HALF:j * HALF, :].astype(F32)
        yf[pl.ds(keep, HALF), cols] = part
        psend[(j - 1) * HALF:j * HALF, :] = part.astype(BF16)
        for s, dev in enumerate((nd, nx, ny)):
            remote(psend.at[pl.ds((j - 1) * HALF + piece(dev), PIECE), :], precv.at[pl.ds(((j - 1) * 3 + s) * PIECE, PIECE), :],
                   rs_s, rs_r, dev).start()

    bytes_in = hid.at[pl.ds(0, (7 * JW + 3 * (D - JW)) * PIECE // D), :]
    rs_all = remote(bytes_in, bytes_in, rs_s, rs_r, nx)
    rs_all.wait_recv()
    mine = rows_of(me)
    y0 = yf[pl.ds(mine, PIECE), 0:JW]
    for k in range(7):
        y0 = y0 + precv0[k * PIECE:(k + 1) * PIECE, :].astype(F32)
    ys = [y0]
    for j in range(1, NJ):
        yj = yf[pl.ds(mine, PIECE), j * JW:(j + 1) * JW]
        for s in range(3):
            row = ((j - 1) * 3 + s) * PIECE
            yj = yj + precv[row:row + PIECE, :].astype(F32)
        ys.append(yj)
    y = jnp.concatenate(ys, axis=-1)
    res = hid[pl.ds(mine, PIECE), :].astype(F32) + y
    inv_rms = lax.rsqrt(jnp.mean(res * res, axis=-1, keepdims=True) + NORM_EPS)
    xbuf[0:PIECE, :] = (gain[...] * res * inv_rms).astype(BF16)

    def xrow(k):
        return xbuf.at[pl.ds(POS[k] * PIECE, PIECE), :]

    for s, k in enumerate((6, 2, 4)):
        remote(xrow(0), xrow(k), x_s, xa_r.at[s], me ^ k).start()
    remote(xrow(0), xrow(1), x_s, xf_r, pt).start()

    def place(dev, i):
        row = pl.multiple_of((dev * 2 + i // GRID) * 128, 128)
        col = pl.multiple_of((i % GRID) * CW, CW)
        return row, pl.ds(col, CW)

    def block(dev, i, first, count, chunks=1):
        row, _ = place(dev, i)
        col = pl.multiple_of((i % GRID) * CW, CW)
        return w.at[pl.ds(row + first, count), pl.ds(col, chunks * CW)]

    def own_start(i, first, count, chunks=1):
        ref = block(me, i, first, count, chunks)
        remote(ref, ref, bulk_s, rxy.at[i // 2], nx).start()
        remote(ref, ref, bulk_s, rxy.at[i // 2], ny).start()
        remote(ref, ref, bulk_s, pr.at[i // 2], pt).start()

    def logits(i, first, count):
        acc = jnp.dot(xbuf[first:first + count, :], wv[:, pl.ds(pl.multiple_of(i * CW, CW), CW)], preferred_element_type=F32)
        scale = invt[first:first + count, :]
        return [acc[:, q * 128:(q + 1) * 128] * scale for q in range(CW // 128)]

    def row_max(parts):
        top = parts[0]
        for p in parts[1:]:
            top = jnp.maximum(top, p)
        return jnp.max(top, axis=-1, keepdims=True)

    def put(i, first, count, parts, top):
        row, _ = place(me, i)
        for q, p in enumerate(parts):
            w[pl.ds(row + first, count), pl.ds(pl.multiple_of((i % GRID) * CW + q * 128, 128), 128)] = (p - top).astype(BF16)

    def statistics(i, first, count, parts, top):
        total = weighted = hit = jnp.zeros((count, 128), F32)
        lane = lax.broadcasted_iota(jnp.int32, (count, 128), 1)
        ids = tgtm[first:first + count, :] - (me * VL + i * CW)
        for q, p in enumerate(parts):
            e = jnp.exp(p - top)
            total = total + e
            weighted = weighted + e * p
            hit = hit + jnp.where(ids == lane + q * 128, p, 0.0)
        sm = statm[first:first + count, :]
        sm = jnp.where(lane == i, top, sm)
        sm = jnp.where(lane == 16 + i, jnp.sum(total, axis=-1, keepdims=True), sm)
        sm = jnp.where(lane == 32 + i, jnp.sum(weighted, axis=-1, keepdims=True), sm)
        sm = jnp.where(lane == 48 + i, jnp.sum(hit, axis=-1, keepdims=True), sm)
        statm[first:first + count, :] = sm

    def head(i, first, count, go=False):
        parts = logits(i, first, count)
        top = row_max(parts)
        put(i, first, count, parts, top)
        if go:
            own_start(i, first, count)
        elif first:
            @pl.when(i < EARLY)
            def _():
                own_start(i, first, count)

        statistics(i, first, count, parts, top)

    def head_rest(i, _):
        head(i, PIECE, B - PIECE)
        return 0

    def head_all(i, _):
        head(i, 0, B)
        return 0

    def own_statistics(i, _):
        parts = [kept[:, pl.ds(pl.multiple_of(i * CW + q * 128, 128), 128)] for q in range(CW // 128)]
        statistics(i, 0, PIECE, parts, row_max(parts))
        return 0

    ready = 0
    for start in range(0, OWN, GROUP):
        group = range(start, min(start + GROUP, OWN))
        while ready * WW < (group[-1] + 1) * CW:
            wv_copies[ready].wait()
            ready += 1
        for i, parts in [(i, logits(i, 0, PIECE)) for i in group]:
            put(i, 0, PIECE, parts, row_max(parts))
            for q, p in enumerate(parts):
                kept[:, i * CW + q * 128:i * CW + (q + 1) * 128] = p
        own_start(start, 0, PIECE, len(group))
    for s, k in ((1, 2), (2, 4), (0, 6)):
        remote(xrow(k), xrow(k), x_s, xa_r.at[s], me ^ k).wait_recv()
        remote(xrow(k), xrow(k + 1), x_s, xf_r, pt).start()
    head(0, PIECE, HALF - PIECE, True)
    four = xbuf.at[pl.ds(0, 4 * PIECE), :]
    remote(four, four, x_s, xf_r, pt).wait_recv()
    head(0, HALF, HALF, True)
    for c in wv_copies[ready:]:
        c.wait()
    lax.fori_loop(1, OWN, head_rest, 0)
    lax.fori_loop(OWN, NC, head_all, 0)
    lax.fori_loop(0, OWN, own_statistics, 0)

    for p, k in enumerate(ORDER):
        offs[pl.ds(rows_of(me ^ k), PIECE), :] = statm[p * PIECE:(p + 1) * PIECE, :]
    st = jnp.transpose(offs[...])
    tops = st[0:NC, :]
    top = jnp.max(tops, axis=0, keepdims=True)
    scale = jnp.exp(tops - top)
    my_stats = jnp.concatenate(
        [tops, top, jnp.sum(scale * st[16:16 + NC, :], axis=0, keepdims=True),
         jnp.sum(scale * st[32:32 + NC, :], axis=0, keepdims=True),
         jnp.sum(st[48:48 + NC, :], axis=0, keepdims=True),
         jnp.zeros((16 - NC - 4, 128), F32)], axis=0)

    stats[0:16, :] = my_stats
    for k in range(1, 8):
        remote(stats.at[pl.ds(0, 16), :], stats.at[pl.ds(16 * k, 16), :], st_s, st_r, me ^ k).start()

    for i in range(EARLY, NC, 2):
        if i + 1 < OWN:
            own_start(i, PIECE, B - PIECE, 2)
        else:
            for n in (i, i + 1):
                own_start(n, PIECE if n < OWN else 0, B - PIECE if n < OWN else B)

    others = stats.at[pl.ds(16, 112), :]
    st_all = remote(others, others, st_s, st_r, nx)
    st_all.wait_recv()
    allst = [stats[16 * k:16 * (k + 1), :] for k in range(8)]
    top = allst[0][NC:NC + 1, :]
    for s in allst[1:]:
        top = jnp.maximum(top, s[NC:NC + 1, :])
    total = weighted = hit = jnp.zeros((1, 128), F32)
    for s in allst:
        scale = jnp.exp(s[NC:NC + 1, :] - top)
        total = total + scale * s[NC + 1:NC + 2, :]
        weighted = weighted + scale * s[NC + 2:NC + 3, :]
        hit = hit + s[NC + 3:NC + 4, :]
    log_norm = top + jnp.log(total)
    small[0:1, :] = log_norm
    small[1:2, :] = log_norm - weighted / total
    small[2:3, :] = hit - log_norm
    small[3:8, :] = jnp.zeros((5, 128), F32)
    offs[...] = jnp.transpose(stats[...] - log_norm)

    lane16 = lax.broadcasted_iota(jnp.int32, (PIECE, 128), 1)

    def fix(rel, i, first=0, count=8):
        dev = me ^ rel
        row, cols = place(dev, i)
        for k in range(first, first + count):
            rows = pl.ds(rows_of(dev ^ ORDER[k]), PIECE)
            off = jnp.sum(jnp.where(lane16 == rel * 16 + i, offs[rows, :], 0.0), axis=-1, keepdims=True)
            val = w[pl.ds(row + k * PIECE, PIECE), cols].astype(F32) + off
            out[rows, pl.ds(pl.multiple_of(dev * VL + i * CW, CW), CW)] = val.astype(BF16)

    def arrived(n, sem):
        ref = w.at[pl.ds(0, n * PIECE), pl.ds(0, CW)]
        remote(ref, ref, bulk_s, sem, nx).wait_recv()

    def send(ref, sem, to):
        remote(ref, ref, bulk_s, sem, to).start()

    def both(rel, p):
        fix(rel, 2 * p)
        fix(rel, 2 * p + 1)

    def arrivals(p, _):
        arrived(32, rxy.at[p])
        if isinstance(p, int):
            for n in range(NS):
                first, count = CUTS[n] * PIECE, (CUTS[n + 1] - CUTS[n]) * PIECE
                for rel, i, to in ((2, 2 * p, ny), (4, 2 * p + 1, nx)):
                    ref = block(me ^ rel, i, first, count)
                    send(ref, rdl.at[n], to)
                    if n == NS - 1:
                        send(ref, prdl.at[n], to ^ 1)
        else:
            send(block(nx, 2 * p, 0, B), rd.at[p], ny)
            send(block(ny, 2 * p + 1, 0, B), rd.at[p], nx)
        send(block(nx, 2 * p, 0, B, 2), pr.at[p], pt)
        send(block(ny, 2 * p, 0, B, 2), pr.at[p], pt)
        both(0, p)
        both(2, p)
        both(4, p)
        arrived(48, pr.at[p])
        both(1, p)
        both(3, p)
        both(5, p)
        return 0

    lax.fori_loop(0, NP - 1, arrivals, 0)
    arrivals(NP - 1, 0)

    for p in range(NP - 1):
        arrived(16, rd.at[p])
        send(block(nd, 2 * p, 0, B, 2), prd.at[p], pt)
        both(6, p)
        if p:
            arrived(16, prd.at[p - 1])
            both(7, p - 1)
    for n in range(NS):
        count = CUTS[n + 1] - CUTS[n]
        arrived(2 * count, rdl.at[n])
        if n < NS - 1:
            send(block(nd, NC - 2, CUTS[n] * PIECE, count * PIECE, 2), prdl.at[n], pt)
        for i in (NC - 2, NC - 1):
            fix(6, i, CUTS[n], count)
        if n == 0:
            arrived(16, prd.at[NP - 2])
            both(7, NP - 2)
    for n in range(NS):
        count = CUTS[n + 1] - CUTS[n]
        arrived(2 * count, prdl.at[n])
        for i in (NC - 2, NC - 1):
            fix(7, i, CUTS[n], count)

    def left(ref, sem):
        remote(ref, ref, sem, rs_r, nx).wait_send()

    left(ysend, d2d_s)
    rs_all.wait_send()
    left(xbuf.at[pl.ds(0, 7 * PIECE), :], x_s)
    st_all.wait_send()
    left(w.at[pl.ds(0, 1792), :], bulk_s)


def _write(src, small, out, o0, o1, o2, sem):
    step = B // 16
    cs = [pltpu.make_async_copy(small.at[pl.ds(k, 1), :], o, sem.at[k]) for k, o in enumerate((o0, o1, o2))]
    for k in range(16):
        for c in range(4):
            at = (pl.ds(k * step, step), pl.ds(c * (V // 4), V // 4))
            pltpu.make_async_copy(src.at[at], out.at[at], sem.at[3]).start()
    for c in cs:
        c.start()
    for c in cs:
        c.wait()
    pltpu.make_async_copy(src, out, sem.at[3]).wait()


def solution(mesh):
    vmem = pl.BlockSpec(memory_space=pltpu.VMEM)
    hbm = pl.BlockSpec(memory_space=pltpu.HBM)
    dma = pltpu.SemaphoreType.DMA

    def device_step(hidden, w_gate, w_up, w_down, norm_gain, w_vocab, temperature, target):
        wide, small = pl.pallas_call(
            _main,
            out_shape=(pltpu.VMEM((B, V), BF16), pltpu.VMEM((8, 128), F32)),
            in_specs=[hbm] * 8,
            out_specs=(vmem, vmem),
            scratch_shapes=[
                pltpu.VMEM((2048, 3072), BF16), pltpu.VMEM((D, VL), BF16), pltpu.VMEM((B, D), BF16),
                pltpu.VMEM((B, FL), BF16), pltpu.VMEM((B, D), F32), pltpu.VMEM((B, JW), BF16), pltpu.VMEM(((NJ - 1) * HALF, JW), BF16),
                pltpu.VMEM(((NJ - 1) * HALF, JW), BF16), pltpu.VMEM(((NJ - 1) * HALF, JW), BF16), pltpu.VMEM((7 * PIECE, JW), BF16),
                pltpu.VMEM(((NJ - 1) * 3 * PIECE, JW), BF16),
                pltpu.VMEM((B, D), BF16), pltpu.VMEM((PIECE, OWN * CW), F32), pltpu.VMEM((128, 128), F32), pltpu.VMEM((128, 128), F32),
                pltpu.VMEM((128, 128), F32), pltpu.VMEM((128, 128), F32), pltpu.VMEM((128, 128), jnp.int32),
                pltpu.VMEM((1, D), F32), pltpu.VMEM((1, B), F32), pltpu.VMEM((1, B), jnp.int32),
                dma((4,)), dma((NF,)), dma((NJ,)), dma((NW,)),
                dma, dma((NJ - 1,)), dma, dma, dma, dma((3,)), dma, dma, dma, dma,
                dma((NP,)), dma((NP - 1,)), dma((NS,)), dma((NP,)), dma((NP - 1,)), dma((NS,)),
            ],
            compiler_params=pltpu.CompilerParams(collective_id=0, has_side_effects=True, vmem_limit_bytes=49 << 20),
            name="step",
        )(hidden, w_gate, w_up, w_down, norm_gain.reshape(1, D), w_vocab, temperature.reshape(1, B), target.reshape(1, B))
        row = jax.ShapeDtypeStruct((1, B), F32)
        log_probs, log_norm, entropy, target_logp = pl.pallas_call(
            _write,
            out_shape=(jax.ShapeDtypeStruct((B, V), BF16), row, row, row),
            in_specs=[vmem, vmem],
            out_specs=(hbm, hbm, hbm, hbm),
            scratch_shapes=[dma((4,))],
            compiler_params=pltpu.CompilerParams(vmem_limit_bytes=16 << 20),
            name="write",
        )(wide, small)
        return log_norm.reshape(B), entropy.reshape(B), target_logp.reshape(B), log_probs

    return jax.shard_map(
        device_step,
        mesh=mesh,
        in_specs=(P("dp", None), P(None, "tp"), P(None, "tp"), P("tp", None), P(None),
                  P(None, "tp"), P("dp"), P("dp")),
        out_specs=(P("dp"), P("dp"), P("dp"), P("dp", None)),
        check_vma=False,
    )
```

```python
import jax
import jax.numpy as jnp
from jax import lax
from jax.experimental import pallas as pl
from jax.experimental.pallas import tpu as pltpu
from jax.sharding import PartitionSpec as P

NORM_EPS = 1e-6
F32 = jnp.float32
BF16 = jnp.bfloat16
B, D, FL, V, VL = 128, 2048, 1024, 49152, 6144
NC = 8
CW = VL // NC
GRID = 3072 // CW
EARLY = 4
OWN = 7
GROUP = 2
NP = NC // 2
CUTS = (0, 6, 7, 8)
NS = len(CUTS) - 1
FCUTS = (0, 256, 768, 1024)
NF = len(FCUTS) - 1
WD_AT = (1, 2, 4)
NJ = 4
JW = D // NJ
HALF, PIECE = 64, 16
NW = 2
WW = VL // NW


ORDER = (0, 2, 4, 6, 1, 3, 5, 7)
POS = tuple(ORDER.index(k) for k in range(8))


def _lanes(row):
    return jnp.transpose(jnp.broadcast_to(row, (128, 128)))


def _main(hid_hbm, wg_hbm, wu_hbm, wd_hbm, gain_hbm, wv_hbm, temp_hbm, tgt_hbm,
          out, small,
          w, wv, hid, act, yf, yall, ysend, yrecv, psend, precv0, precv, xbuf, kept, statm, stats, offs, invt, tgtm, gain, temp, tgt,
          in_sem, wf_sem, wd_sem, wv_sem,
          d2d_s, d2d_r, rs_s, rs_r, x_s, xa_r, xf_r, st_s, st_r, bulk_s, rxy, rd, rdl, pr, prd, prdl):
    me = lax.axis_index("tp")
    core = me % 2
    nx, ny, nd, pt = me ^ 2, me ^ 4, me ^ 6, me ^ 1

    def remote(src, dst, ss, rs, dev):
        return pltpu.make_async_remote_copy(src, dst, ss, rs, device_id={"tp": dev})

    def load(src, dst, sem):
        c = pltpu.make_async_copy(src, dst, sem)
        c.start()
        return c

    def load_wf(b):
        for t, ref in enumerate((wg_hbm, wu_hbm)):
            start, width = FCUTS[b], FCUTS[b + 1] - FCUTS[b]
            load(ref.at[:, pl.ds(start, width)], w.at[:, pl.ds(t * FL + start, width)], wf_sem.at[b])

    def wait_wf(b):
        width = 2 * (FCUTS[b + 1] - FCUTS[b])
        pltpu.make_async_copy(wv_hbm.at[:, pl.ds(0, width)], w.at[:, pl.ds(0, width)], wf_sem.at[b]).wait()

    def load_wd(j):
        return load(wd_hbm.at[:, pl.ds(j * JW, JW)], w.at[pl.ds(j % 2 * FL, FL), pl.ds(2 * FL + j // 2 * JW, JW)], wd_sem.at[j])

    def load_wv(n):
        return load(wv_hbm.at[:, pl.ds(n * WW, WW)], wv.at[:, pl.ds(n * WW, WW)], wv_sem.at[n])

    hid_copy = load(hid_hbm, hid, in_sem.at[0])
    load_wf(0)
    small_copies = [load(temp_hbm, temp, in_sem.at[1]), load(tgt_hbm, tgt, in_sem.at[2]), load(gain_hbm, gain, in_sem.at[3])]
    for b in range(1, NF):
        load_wf(b)

    barrier = pltpu.get_barrier_semaphore()
    for k in range(1, 8):
        pl.semaphore_signal(barrier, inc=1, device_id={"tp": me ^ k})

    hid_copy.wait()
    wd_copies, wv_copies = [], []
    for b in range(NF):
        wait_wf(b)
        for j in range(len(wd_copies), WD_AT[b]):
            wd_copies.append(load_wd(j))
        g = jnp.dot(hid[...], w[:, FCUTS[b]:FCUTS[b + 1]], preferred_element_type=F32)
        u = jnp.dot(hid[...], w[:, FL + FCUTS[b]:FL + FCUTS[b + 1]], preferred_element_type=F32)
        act[:, FCUTS[b]:FCUTS[b + 1]] = (jax.nn.silu(g) * u).astype(BF16)

    def rows_of(dev):
        return pl.multiple_of((dev % 2) * HALF + (dev // 2) * PIECE, PIECE)

    keep = pl.multiple_of(core * HALF, HALF)
    give = pl.multiple_of(HALF - core * HALF, HALF)
    d2d = []
    for j in range(NJ):
        wd_copies[j].wait()
        if j < NW:
            wv_copies.append(load_wv(j))
        wd = w[j % 2 * FL:(j % 2 + 1) * FL, 2 * FL + j // 2 * JW:2 * FL + (j // 2 + 1) * JW]
        yf[:, j * JW:(j + 1) * JW] = jnp.dot(act[...], wd, preferred_element_type=F32)
        if j == 0:
            yall[...] = yf[:, 0:JW].astype(BF16)
            pl.semaphore_wait(barrier, 7)
            for k in (6, 7, 2, 3, 4, 5, 1):
                remote(yall.at[pl.ds(rows_of(me ^ k), PIECE), :], precv0.at[pl.ds((k - 1) * PIECE, PIECE), :],
                       rs_s, rs_r, me ^ k).start()
            continue
        rows = pl.ds((j - 1) * HALF, HALF)
        ysend[rows, :] = yf[pl.ds(give, HALF), j * JW:(j + 1) * JW].astype(BF16)
        c = remote(ysend.at[rows, :], yrecv.at[rows, :], d2d_s, d2d_r.at[j - 1], pt)
        c.start()
        d2d.append(c)

    for n in range(min(NJ, NW), NW):
        wv_copies.append(load_wv(n))
    for c in small_copies:
        c.wait()
    offs[...] = _lanes(1.0 / temp[...])
    statm[...] = _lanes(tgt[...].astype(F32))
    for p, k in enumerate(ORDER):
        rows = pl.ds(rows_of(me ^ k), PIECE)
        invt[p * PIECE:(p + 1) * PIECE, :] = offs[rows, :]
        tgtm[p * PIECE:(p + 1) * PIECE, :] = statm[rows, :].astype(jnp.int32)

    def piece(dev):
        return pl.multiple_of((dev // 2) * PIECE, PIECE)

    for j in range(1, NJ):
        cols = slice(j * JW, (j + 1) * JW)
        d2d[j - 1].wait_recv()
        part = yf[pl.ds(keep, HALF), cols] + yrecv[(j - 1) * HALF:j * HALF, :].astype(F32)
        yf[pl.ds(keep, HALF), cols] = part
        psend[(j - 1) * HALF:j * HALF, :] = part.astype(BF16)
        for s, dev in enumerate((nd, nx, ny)):
            remote(psend.at[pl.ds((j - 1) * HALF + piece(dev), PIECE), :], precv.at[pl.ds(((j - 1) * 3 + s) * PIECE, PIECE), :],
                   rs_s, rs_r, dev).start()

    bytes_in = hid.at[pl.ds(0, (7 * JW + 3 * (D - JW)) * PIECE // D), :]
    rs_all = remote(bytes_in, bytes_in, rs_s, rs_r, nx)
    rs_all.wait_recv()
    mine = rows_of(me)
    y0 = yf[pl.ds(mine, PIECE), 0:JW]
    for k in range(7):
        y0 = y0 + precv0[k * PIECE:(k + 1) * PIECE, :].astype(F32)
    ys = [y0]
    for j in range(1, NJ):
        yj = yf[pl.ds(mine, PIECE), j * JW:(j + 1) * JW]
        for s in range(3):
            row = ((j - 1) * 3 + s) * PIECE
            yj = yj + precv[row:row + PIECE, :].astype(F32)
        ys.append(yj)
    y = jnp.concatenate(ys, axis=-1)
    res = hid[pl.ds(mine, PIECE), :].astype(F32) + y
    inv_rms = lax.rsqrt(jnp.mean(res * res, axis=-1, keepdims=True) + NORM_EPS)
    xbuf[0:PIECE, :] = (gain[...] * res * inv_rms).astype(BF16)

    def xrow(k):
        return xbuf.at[pl.ds(POS[k] * PIECE, PIECE), :]

    for s, k in enumerate((6, 2, 4)):
        remote(xrow(0), xrow(k), x_s, xa_r.at[s], me ^ k).start()
    remote(xrow(0), xrow(1), x_s, xf_r, pt).start()

    def place(dev, i):
        row = pl.multiple_of((dev * 2 + i // GRID) * 128, 128)
        col = pl.multiple_of((i % GRID) * CW, CW)
        return row, pl.ds(col, CW)

    def block(dev, i, first, count, chunks=1):
        row, _ = place(dev, i)
        col = pl.multiple_of((i % GRID) * CW, CW)
        return w.at[pl.ds(row + first, count), pl.ds(col, chunks * CW)]

    def own_start(i, first, count, chunks=1):
        ref = block(me, i, first, count, chunks)
        remote(ref, ref, bulk_s, rxy.at[i // 2], nx).start()
        remote(ref, ref, bulk_s, rxy.at[i // 2], ny).start()
        remote(ref, ref, bulk_s, pr.at[i // 2], pt).start()

    def logits(i, first, count):
        acc = jnp.dot(xbuf[first:first + count, :], wv[:, pl.ds(pl.multiple_of(i * CW, CW), CW)], preferred_element_type=F32)
        scale = invt[first:first + count, :]
        return [acc[:, q * 128:(q + 1) * 128] * scale for q in range(CW // 128)]

    def row_max(parts):
        top = parts[0]
        for p in parts[1:]:
            top = jnp.maximum(top, p)
        return jnp.max(top, axis=-1, keepdims=True)

    def put(i, first, count, parts, top):
        row, _ = place(me, i)
        for q, p in enumerate(parts):
            w[pl.ds(row + first, count), pl.ds(pl.multiple_of((i % GRID) * CW + q * 128, 128), 128)] = (p - top).astype(BF16)

    def statistics(i, first, count, parts, top):
        total = weighted = hit = jnp.zeros((count, 128), F32)
        lane = lax.broadcasted_iota(jnp.int32, (count, 128), 1)
        ids = tgtm[first:first + count, :] - (me * VL + i * CW)
        for q, p in enumerate(parts):
            e = jnp.exp(p - top)
            total = total + e
            weighted = weighted + e * p
            hit = hit + jnp.where(ids == lane + q * 128, p, 0.0)
        sm = statm[first:first + count, :]
        sm = jnp.where(lane == i, top, sm)
        sm = jnp.where(lane == 16 + i, jnp.sum(total, axis=-1, keepdims=True), sm)
        sm = jnp.where(lane == 32 + i, jnp.sum(weighted, axis=-1, keepdims=True), sm)
        sm = jnp.where(lane == 48 + i, jnp.sum(hit, axis=-1, keepdims=True), sm)
        statm[first:first + count, :] = sm

    def head(i, first, count, go=False):
        parts = logits(i, first, count)
        top = row_max(parts)
        put(i, first, count, parts, top)
        if go:
            own_start(i, first, count)
        elif first:
            @pl.when(i < EARLY)
            def _():
                own_start(i, first, count)

        statistics(i, first, count, parts, top)

    def head_rest(i, _):
        head(i, PIECE, B - PIECE)
        return 0

    def head_all(i, _):
        head(i, 0, B)
        return 0

    def own_statistics(i, _):
        parts = [kept[:, pl.ds(pl.multiple_of(i * CW + q * 128, 128), 128)] for q in range(CW // 128)]
        statistics(i, 0, PIECE, parts, row_max(parts))
        return 0

    ready = 0
    for start in range(0, OWN, GROUP):
        group = range(start, min(start + GROUP, OWN))
        while ready * WW < (group[-1] + 1) * CW:
            wv_copies[ready].wait()
            ready += 1
        for i, parts in [(i, logits(i, 0, PIECE)) for i in group]:
            put(i, 0, PIECE, parts, row_max(parts))
            for q, p in enumerate(parts):
                kept[:, i * CW + q * 128:i * CW + (q + 1) * 128] = p
        own_start(start, 0, PIECE, len(group))
    for s, k in ((1, 2), (2, 4), (0, 6)):
        remote(xrow(k), xrow(k), x_s, xa_r.at[s], me ^ k).wait_recv()
        remote(xrow(k), xrow(k + 1), x_s, xf_r, pt).start()
    head(0, PIECE, HALF - PIECE, True)
    four = xbuf.at[pl.ds(0, 4 * PIECE), :]
    remote(four, four, x_s, xf_r, pt).wait_recv()
    head(0, HALF, HALF, True)
    for c in wv_copies[ready:]:
        c.wait()
    lax.fori_loop(1, OWN, head_rest, 0)
    lax.fori_loop(OWN, NC, head_all, 0)
    lax.fori_loop(0, OWN, own_statistics, 0)

    for p, k in enumerate(ORDER):
        offs[pl.ds(rows_of(me ^ k), PIECE), :] = statm[p * PIECE:(p + 1) * PIECE, :]
    st = jnp.transpose(offs[...])
    tops = st[0:NC, :]
    top = jnp.max(tops, axis=0, keepdims=True)
    scale = jnp.exp(tops - top)
    my_stats = jnp.concatenate(
        [tops, top, jnp.sum(scale * st[16:16 + NC, :], axis=0, keepdims=True),
         jnp.sum(scale * st[32:32 + NC, :], axis=0, keepdims=True),
         jnp.sum(st[48:48 + NC, :], axis=0, keepdims=True),
         jnp.zeros((16 - NC - 4, 128), F32)], axis=0)

    stats[0:16, :] = my_stats
    for k in range(1, 8):
        remote(stats.at[pl.ds(0, 16), :], stats.at[pl.ds(16 * k, 16), :], st_s, st_r, me ^ k).start()

    for i in range(EARLY, NC, 2):
        if i + 1 < OWN:
            own_start(i, PIECE, B - PIECE, 2)
        else:
            for n in (i, i + 1):
                own_start(n, PIECE if n < OWN else 0, B - PIECE if n < OWN else B)

    others = stats.at[pl.ds(16, 112), :]
    st_all = remote(others, others, st_s, st_r, nx)
    st_all.wait_recv()
    allst = [stats[16 * k:16 * (k + 1), :] for k in range(8)]
    top = allst[0][NC:NC + 1, :]
    for s in allst[1:]:
        top = jnp.maximum(top, s[NC:NC + 1, :])
    total = weighted = hit = jnp.zeros((1, 128), F32)
    for s in allst:
        scale = jnp.exp(s[NC:NC + 1, :] - top)
        total = total + scale * s[NC + 1:NC + 2, :]
        weighted = weighted + scale * s[NC + 2:NC + 3, :]
        hit = hit + s[NC + 3:NC + 4, :]
    log_norm = top + jnp.log(total)
    small[0:1, :] = log_norm
    small[1:2, :] = log_norm - weighted / total
    small[2:3, :] = hit - log_norm
    small[3:8, :] = jnp.zeros((5, 128), F32)
    offs[...] = jnp.transpose(stats[...] - log_norm)

    lane16 = lax.broadcasted_iota(jnp.int32, (PIECE, 128), 1)

    def fix(rel, i, first=0, count=8):
        dev = me ^ rel
        row, cols = place(dev, i)
        for k in range(first, first + count):
            rows = pl.ds(rows_of(dev ^ ORDER[k]), PIECE)
            off = jnp.sum(jnp.where(lane16 == rel * 16 + i, offs[rows, :], 0.0), axis=-1, keepdims=True)
            val = w[pl.ds(row + k * PIECE, PIECE), cols].astype(F32) + off
            out[rows, pl.ds(pl.multiple_of(dev * VL + i * CW, CW), CW)] = val.astype(BF16)

    def arrived(n, sem):
        ref = w.at[pl.ds(0, n * PIECE), pl.ds(0, CW)]
        remote(ref, ref, bulk_s, sem, nx).wait_recv()

    def send(ref, sem, to):
        remote(ref, ref, bulk_s, sem, to).start()

    def both(rel, p):
        fix(rel, 2 * p)
        fix(rel, 2 * p + 1)

    def arrivals(p, _):
        arrived(32, rxy.at[p])
        if isinstance(p, int):
            for n in range(NS):
                first, count = CUTS[n] * PIECE, (CUTS[n + 1] - CUTS[n]) * PIECE
                for rel, i, to in ((2, 2 * p, ny), (4, 2 * p + 1, nx)):
                    ref = block(me ^ rel, i, first, count)
                    send(ref, rdl.at[n], to)
                    if n == NS - 1:
                        send(ref, prdl.at[n], to ^ 1)
        else:
            send(block(nx, 2 * p, 0, B), rd.at[p], ny)
            send(block(ny, 2 * p + 1, 0, B), rd.at[p], nx)
        send(block(nx, 2 * p, 0, B, 2), pr.at[p], pt)
        send(block(ny, 2 * p, 0, B, 2), pr.at[p], pt)
        both(0, p)
        both(2, p)
        both(4, p)
        arrived(48, pr.at[p])
        both(1, p)
        both(3, p)
        both(5, p)
        return 0

    lax.fori_loop(0, NP - 1, arrivals, 0)
    arrivals(NP - 1, 0)

    for p in range(NP - 1):
        arrived(16, rd.at[p])
        send(block(nd, 2 * p, 0, B, 2), prd.at[p], pt)
        both(6, p)
        if p:
            arrived(16, prd.at[p - 1])
            both(7, p - 1)
    for n in range(NS):
        count = CUTS[n + 1] - CUTS[n]
        arrived(2 * count, rdl.at[n])
        if n < NS - 1:
            send(block(nd, NC - 2, CUTS[n] * PIECE, count * PIECE, 2), prdl.at[n], pt)
        for i in (NC - 2, NC - 1):
            fix(6, i, CUTS[n], count)
        if n == 0:
            arrived(16, prd.at[NP - 2])
            both(7, NP - 2)
    for n in range(NS):
        count = CUTS[n + 1] - CUTS[n]
        arrived(2 * count, prdl.at[n])
        for i in (NC - 2, NC - 1):
            fix(7, i, CUTS[n], count)

    def left(ref, sem):
        remote(ref, ref, sem, rs_r, nx).wait_send()

    left(ysend, d2d_s)
    rs_all.wait_send()
    left(xbuf.at[pl.ds(0, 7 * PIECE), :], x_s)
    st_all.wait_send()
    left(w.at[pl.ds(0, 1792), :], bulk_s)


def _write(src, small, out, o0, o1, o2, sem):
    step = B // 16
    cs = [pltpu.make_async_copy(small.at[pl.ds(k, 1), :], o, sem.at[k]) for k, o in enumerate((o0, o1, o2))]
    for k in range(16):
        for c in range(8):
            at = (pl.ds(k * step, step), pl.ds(c * (V // 8), V // 8))
            pltpu.make_async_copy(src.at[at], out.at[at], sem.at[3]).start()
    for c in cs:
        c.start()
    for c in cs:
        c.wait()
    pltpu.make_async_copy(src, out, sem.at[3]).wait()


def solution(mesh):
    vmem = pl.BlockSpec(memory_space=pltpu.VMEM)
    hbm = pl.BlockSpec(memory_space=pltpu.HBM)
    dma = pltpu.SemaphoreType.DMA

    def device_step(hidden, w_gate, w_up, w_down, norm_gain, w_vocab, temperature, target):
        wide, small = pl.pallas_call(
            _main,
            out_shape=(pltpu.VMEM((B, V), BF16), pltpu.VMEM((8, 128), F32)),
            in_specs=[hbm] * 8,
            out_specs=(vmem, vmem),
            scratch_shapes=[
                pltpu.VMEM((2048, 3072), BF16), pltpu.VMEM((D, VL), BF16), pltpu.VMEM((B, D), BF16),
                pltpu.VMEM((B, FL), BF16), pltpu.VMEM((B, D), F32), pltpu.VMEM((B, JW), BF16), pltpu.VMEM(((NJ - 1) * HALF, JW), BF16),
                pltpu.VMEM(((NJ - 1) * HALF, JW), BF16), pltpu.VMEM(((NJ - 1) * HALF, JW), BF16), pltpu.VMEM((7 * PIECE, JW), BF16),
                pltpu.VMEM(((NJ - 1) * 3 * PIECE, JW), BF16),
                pltpu.VMEM((B, D), BF16), pltpu.VMEM((PIECE, OWN * CW), F32), pltpu.VMEM((128, 128), F32), pltpu.VMEM((128, 128), F32),
                pltpu.VMEM((128, 128), F32), pltpu.VMEM((128, 128), F32), pltpu.VMEM((128, 128), jnp.int32),
                pltpu.VMEM((1, D), F32), pltpu.VMEM((1, B), F32), pltpu.VMEM((1, B), jnp.int32),
                dma((4,)), dma((NF,)), dma((NJ,)), dma((NW,)),
                dma, dma((NJ - 1,)), dma, dma, dma, dma((3,)), dma, dma, dma, dma,
                dma((NP,)), dma((NP - 1,)), dma((NS,)), dma((NP,)), dma((NP - 1,)), dma((NS,)),
            ],
            compiler_params=pltpu.CompilerParams(collective_id=0, has_side_effects=True, vmem_limit_bytes=49 << 20),
            name="step",
        )(hidden, w_gate, w_up, w_down, norm_gain.reshape(1, D), w_vocab, temperature.reshape(1, B), target.reshape(1, B))
        row = jax.ShapeDtypeStruct((1, B), F32)
        log_probs, log_norm, entropy, target_logp = pl.pallas_call(
            _write,
            out_shape=(jax.ShapeDtypeStruct((B, V), BF16), row, row, row),
            in_specs=[vmem, vmem],
            out_specs=(hbm, hbm, hbm, hbm),
            scratch_shapes=[dma((4,))],
            compiler_params=pltpu.CompilerParams(vmem_limit_bytes=16 << 20),
            name="write",
        )(wide, small)
        return log_norm.reshape(B), entropy.reshape(B), target_logp.reshape(B), log_probs

    return jax.shard_map(
        device_step,
        mesh=mesh,
        in_specs=(P("dp", None), P(None, "tp"), P(None, "tp"), P("tp", None), P(None),
                  P(None, "tp"), P("dp"), P("dp")),
        out_specs=(P("dp"), P("dp"), P("dp"), P("dp", None)),
        check_vma=False,
    )
```
